32 devices in a mesh: shear: 16 (over z, y, x), cross: 2 (over core).
Axes of the slice: x: 2, y: 2, z: 4, core: 2. Of those that a mesh axis runs over, the one named last changes fastest.
Arguments:
- positions: float32 [3, 16, 16, 2, 256], P(None, 'shear', None, 'cross'), may hold values from 0 to 1
- masses: float32 [16, 16, 2, 256], P('shear', None, 'cross'), may hold values from 0.002 to 0.008
- counts: int32 [16, 16, 2], P('shear', None, 'cross'), may hold values from 32 to 256
- shear_offset: int32 [1], replicated, may hold values from 0 to 15
Outputs:
- density: float32 [16, 16, 2, 256], P('shear', None, 'cross')
The draws below stay inside these ranges and needn't reach their ends.
Inputs may be any that keep to these rules, and one draw needn't show every extreme that they name: `shear_offset`: a whole number of cells.
All inputs are finite; a program needn't handle non-finite values.
Results may differ from the reference program's by a relative error of at most 0.0003.
Values sent between devices are 32-bit elements; how exact they have to be, the bound alone decides.
A program may use at most 64 MiB of HBM per device.

```python
import math
import jax
import jax.numpy as jnp
from jax import lax

P_SIZE = 256
NX = 16
NY = 16
NZ = 2


def place_ends(entries, stream_key, least, largest):
    index_at = [jax.random.randint(jax.random.fold_in(stream_key, axis), (), 0, length) for axis, length in enumerate(entries.shape)]
    main_axis = entries.shape.index(max(entries.shape))
    next_to = index_at[:main_axis] + [(index_at[main_axis] + 1) % entries.shape[main_axis]] + index_at[main_axis + 1:]
    return entries.at[tuple(index_at)].set(least).at[tuple(next_to)].set(largest)


def level_of(own_key, dims, pieces, least, largest):
    level = 1.0
    for position, blocks in pieces:
        heights = jax.random.uniform(jax.random.fold_in(jax.random.fold_in(own_key, 6), position), (blocks,), jnp.float32, least / len(pieces), largest / len(pieces))
        level = level * jnp.repeat(jnp.exp(heights), dims[position] // blocks).reshape((-1,) + (1,) * (len(dims) - 1 - position))
    return level


def setup_inputs(seed: int = 0) -> dict:
    splits = jax.random.split(jax.random.key(seed), 5)
    positions = jnp.clip(1.0 * jax.random.uniform(splits[0], (3, NY, NX, NZ, P_SIZE), jnp.float32) ** level_of(splits[0], (3, NY, NX, NZ, P_SIZE), ((1, 16), (3, 2)), -0.2, 0.2), 0.0, 1.0)
    masses = jnp.clip(jnp.exp(math.log(0.008) - 1.3862944 * jax.random.uniform(splits[1], (NY, NX, NZ, P_SIZE), jnp.float32) ** level_of(splits[1], (NY, NX, NZ, P_SIZE), ((0, 16), (2, 2)), -0.2, 0.2)), 0.002, 0.008)
    counts = place_ends(jax.random.randint(splits[2], (NY, NX, NZ), P_SIZE // 8, P_SIZE + 1), jax.random.fold_in(splits[2], 1), P_SIZE // 8, P_SIZE).astype(jnp.int32)
    shear_offset = jax.random.randint(splits[3], (1,), 0, NX).astype(jnp.int32)
    return dict(positions=positions, masses=masses, counts=counts, shear_offset=shear_offset)


def spline(squared):
    radius = jnp.sqrt(squared) * 4.0
    inner_part = 1.0 - 1.5 * radius * radius + 0.75 * radius * radius * radius
    outer_part = 0.25 * jnp.maximum(2.0 - radius, 0.0) ** 3
    return jnp.where(radius < 1.0, inner_part, outer_part) * (64.0 / 3.141592653589793)

def distance_sq(target, source_pos, offset_vec):
    squared = None
    for component in range(3):
        moved = source_pos[component] + offset_vec[component]
        gap = target[component][..., :, None] - moved[..., None, :]
        squared = gap * gap if squared is None else squared + gap * gap
    return squared

def reference(positions, masses, counts, shear_offset):
    slot_index = lax.broadcasted_iota(jnp.int32, masses.shape, 3)
    is_valid = slot_index < counts[..., None]
    weight = jnp.where(is_valid, masses, jnp.float32(0.0))
    particle_data = jnp.concatenate([positions, weight[None]], 0)
    offset = shear_offset[0]
    top_row = jnp.roll(particle_data[:, 0:1], -offset, axis=2)
    bottom_row = jnp.roll(particle_data[:, -1:], offset, axis=2)
    extended = jnp.concatenate([bottom_row, particle_data, top_row], 1)
    extended = jnp.concatenate([extended[:, :, :, -1:], extended, extended[:, :, :, :1]], 3)
    width_z = masses.shape[2]

    def row_density(row_at):
        band = lax.dynamic_slice_in_dim(extended, row_at, 3, 1)
        target = band[:3, 1, :, 1:1 + width_z]
        density = jnp.zeros(target.shape[1:], jnp.float32)
        for step_y in (-1, 0, 1):
            for step_z in (-1, 0, 1):
                for step_x in (-1, 0, 1):
                    source_cells = jnp.roll(band[:, 1 + step_y, :, 1 + step_z:1 + step_z + width_z], -step_x, axis=1)
                    offset_vec = (float(step_y), float(step_x), float(step_z))
                    kernel = spline(distance_sq(target, source_cells[:3], offset_vec))
                    density = density + lax.optimization_barrier(jnp.sum(kernel * source_cells[3][..., None, :], axis=-1))
        valid_row = lax.dynamic_index_in_dim(is_valid, row_at, 0, keepdims=False)
        return jnp.where(valid_row, density, jnp.float32(0.0))
    return lax.map(row_density, jnp.arange(masses.shape[0], dtype=jnp.int32))
```

```python
import functools
import jax
import jax.numpy as jnp
from jax import lax
from jax.experimental import pallas as pl
from jax.experimental.pallas import tpu as pltpu
from jax.sharding import PartitionSpec as P

LANES = 128
SUB = 8
GROUPS = 8
RODS = ((0, 0), (0, 1), (1, 0), (1, 1))


def halo_kernel(data_ref, out_ref, send_sems, recv_sems, local_sem):
    shear, cross = lax.axis_index("shear"), lax.axis_index("cross")
    rows, planes = lax.axis_size("shear"), lax.axis_size("cross")
    mesh_ids = pl.DeviceIdType.MESH
    along_y = [(lax.rem(shear + rows - step, rows), cross) for step in (-1, 1)]
    along_z = [(shear, lax.rem(cross + planes - step, planes)) for step in (-1, 1)]
    barrier = pltpu.get_barrier_semaphore()
    for device in along_y + along_z:
        pl.semaphore_signal(barrier, inc=1, device_id=device, device_id_type=mesh_ids)
    own = pltpu.make_async_copy(data_ref, out_ref.at[1, 1], local_sem)
    own.start()
    pl.semaphore_wait(barrier, 4)

    def sent(source, y, z, device):
        slot = 3 * y + z
        copy = pltpu.make_async_remote_copy(
            src_ref=source,
            dst_ref=out_ref.at[y, z],
            send_sem=send_sems.at[slot],
            recv_sem=recv_sems.at[slot],
            device_id=device,
            device_id_type=mesh_ids,
        )
        copy.start()
        return copy

    rows_sent = [sent(data_ref, y, 1, along_y[k]) for k, y in enumerate((0, 2))]
    planes_sent = [sent(data_ref, 1, z, along_z[k]) for k, z in enumerate((0, 2))]
    for k, y in enumerate((0, 2)):
        rows_sent[k].wait_recv()
        for j, z in enumerate((0, 2)):
            planes_sent.append(sent(out_ref.at[y, 1], y, z, along_z[j]))
    for copy in rows_sent:
        copy.wait_send()
    for copy in planes_sent:
        copy.wait()
    own.wait()


def halo(data):
    vmem = pl.BlockSpec(memory_space=pltpu.VMEM)
    return pl.pallas_call(
        halo_kernel,
        out_shape=jax.ShapeDtypeStruct((3, 3) + data.shape, data.dtype),
        in_specs=[vmem],
        out_specs=vmem,
        scratch_shapes=[
            pltpu.SemaphoreType.DMA((9,)),
            pltpu.SemaphoreType.DMA((9,)),
            pltpu.SemaphoreType.DMA,
        ],
        compiler_params=pltpu.CompilerParams(collective_id=0, has_side_effects=True),
        name="halo",
    )(data)


def density_kernel(
    cells, roll_ref, data_ref, out_ref,
    rel_ref, source_ref, place_ref, target_ref, acc_ref, sums_ref, list_ref, list_sm, list_sem,
):
    f32, i32 = jnp.float32, jnp.int32
    tiles = data_ref.shape[3] // cells
    slots = tiles * LANES
    wide = 4 * tiles
    list_tiles = list_ref.shape[0] - 2
    half = 0.5

    masks = {}
    for sy in (-1, 0, 1):
        for sz in (-1, 0, 1):
            relation = 3 * (sy + 1) + sz + 1
            parts = []
            for k in range(4):
                value = jnp.concatenate(
                    [data_ref[sy + 1, sz + 1, k, pl.ds(t, cells, stride=tiles), :] for t in range(tiles)], axis=1
                )
                if sy != 0:
                    value = pltpu.roll(value, roll_ref[(sy + 1) // 2], 0)
                parts.append(value)
            y, x, z, mass = parts
            keep = mass > 0.0
            if sy == -1:
                keep = keep & (y >= half)
            elif sy == 1:
                keep = keep & (y <= half)
            if sz == -1:
                keep = keep & (z >= half)
            elif sz == 1:
                keep = keep & (z <= half)
            masks[sy, sz] = keep
            rel_ref[relation, 0] = 4.0 * (y + (sy - half))
            rel_ref[relation, 1] = 4.0 * (x - half)
            rel_ref[relation, 2] = 4.0 * (z + (sz - half))
            rel_ref[relation, 3] = mass
            if sy == 0 and sz == 0:
                own_y, own_x, own_z, own_valid = y, x, z, keep

    octants = []
    for ry, rz in RODS:
        inside = own_valid & ((own_y >= half) if ry else (own_y < half))
        inside = inside & ((own_z >= half) if rz else (own_z < half))
        octants.append(inside & (own_x < half))
        octants.append(inside & (own_x >= half))

    relations = [(sy, sz) for sy in (-1, 0, 1) for sz in (-1, 0, 1)]
    stacked = jnp.concatenate(
        [jnp.where(masks[r], 1.0, 0.0) for r in relations] + [jnp.where(m, 1.0, 0.0) for m in octants], axis=0
    ).astype(jnp.bfloat16)
    row = lax.broadcasted_iota(i32, (slots, slots + LANES), 0)
    col = lax.broadcasted_iota(i32, (slots, slots + LANES), 1)
    triangle = jnp.where((row <= col) | (col >= slots), 1.0, 0.0).astype(jnp.bfloat16)
    ranks = jnp.dot(stacked, triangle, preferred_element_type=f32).astype(i32)

    first = len(relations) * cells
    totals = ranks[first:, slots:]
    groups = (totals + (SUB - 1)) >> 3
    n_oct = len(octants) * cells
    lower = jnp.where(
        lax.broadcasted_iota(i32, (n_oct, n_oct), 1) < lax.broadcasted_iota(i32, (n_oct, n_oct), 0), 1.0, 0.0
    ).astype(jnp.bfloat16)
    base = jnp.dot(lower, groups.astype(f32).astype(jnp.bfloat16), preferred_element_type=f32).astype(i32)
    end = base + groups
    place = jnp.full((cells, slots), -1, i32)
    for o, inside in enumerate(octants):
        begin = base[o * cells:(o + 1) * cells]
        begin = jnp.concatenate([begin] * tiles, axis=1)
        rank = ranks[first + o * cells:first + (o + 1) * cells, :slots]
        place = jnp.where(inside, SUB * begin + rank - 1, place)
    place_ref[...] = place
    lane = lax.broadcasted_iota(i32, (n_oct, LANES), 1)
    for j in range(list_tiles):
        passed = jnp.where(end <= lane + j * LANES, 1.0, 0.0)
        list_ref[j:j + 1, :] = jnp.minimum(jnp.sum(passed, axis=0, keepdims=True), n_oct - 1.0).astype(i32)
    list_ref[list_tiles:list_tiles + 1, :] = end[n_oct - 1:n_oct]

    lane = lax.broadcasted_iota(i32, (cells, LANES), 1)
    cell_row = lax.broadcasted_iota(i32, (cells, LANES), 0)
    tile_row = jnp.zeros((1, LANES), f32)
    rods = []
    for r, (ry, rz) in enumerate(RODS):
        segments = [(0, 0), (2 * ry - 1, 0), (0, 2 * rz - 1), (2 * ry - 1, 2 * rz - 1)]
        starts, start = [], jnp.zeros((cells, LANES), i32)
        for sy, sz in segments:
            at = (3 * (sy + 1) + sz + 1) * cells
            starts.append(start)
            start = start + ranks[at:at + cells, slots:]
        count = (start + (LANES - 1)) >> 7
        tile_row += jnp.sum(
            jnp.where(lane == cell_row + r * cells, count.astype(f32), 0.0), axis=0, keepdims=True
        )
        rods.append((segments, starts, start))
    list_ref[list_tiles + 1:list_tiles + 2, :] = tile_row.astype(i32)

    lane8 = lax.broadcasted_iota(i32, (SUB, LANES), 1)
    copy = None
    for r, (segments, starts, total) in enumerate(rods):
        for top in range(0, cells, SUB):
            rows = slice(top, top + SUB)
            arrays = [[] for _ in range(4)]
            moves = []
            for k, (sy, sz) in enumerate(segments):
                relation = 3 * (sy + 1) + sz + 1
                for t in range(tiles):
                    lanes = slice(t * LANES, (t + 1) * LANES)
                    for f in range(4):
                        arrays[f].append(rel_ref[relation, f, rows, lanes])
                    if k == 0:
                        moves.append(jnp.zeros((SUB, LANES), i32))
                    else:
                        at = relation * cells + top
                        shift = (k * slots + t * LANES + 1) + lane8 - starts[k][rows] - ranks[at:at + SUB, lanes]
                        moves.append(jnp.where(masks[sy, sz][rows, lanes], shift, 0))
            step = 1
            while step < wide * LANES:
                if step < LANES:
                    inner = lane8 < LANES - step

                    def shifted(values, edge=None):
                        turned = [pltpu.roll(v, LANES - step, 1) for v in values]
                        last = turned[-1] if edge is None else jnp.where(inner, turned[-1], edge)
                        return [jnp.where(inner, a, b) for a, b in zip(turned, turned[1:])] + [last]

                    moved = [shifted(a) for a in arrays]
                    moved_d = shifted(moves, 0)
                    reach = wide
                else:
                    q = step // LANES
                    moved = [a[q:] for a in arrays]
                    moved_d = moves[q:]
                    reach = wide - q
                leaving = [(d & step) != 0 for d in moves]
                coming = [(d & step) != 0 for d in moved_d]
                arrays = [
                    [jnp.where(coming[j], m[j], a[j]) if j < reach else a[j] for j in range(wide)]
                    for m, a in zip(moved, arrays)
                ]
                kept = [jnp.where(leaving[j], 0, moves[j]) for j in range(wide)]
                moves = [jnp.where(coming[j], moved_d[j], kept[j]) if j < reach else kept[j] for j in range(wide)]
                step *= 2
            for j in range(wide):
                for f in range(3):
                    source_ref[(4 * r + f) * wide + j, rows] = arrays[f][j]
                source_ref[(4 * r + 3) * wide + j, rows] = jnp.where(
                    lane8 + j * LANES < total[rows], arrays[3][j], 0.0
                )
        if copy is None:
            copy = pltpu.make_async_copy(list_ref, list_sm, list_sem)
            copy.start()
    copy.wait()

    sub_row = lax.broadcasted_iota(i32, (SUB, slots), 0)
    own = 4

    def entry(g):
        g = jnp.clip(g, 0, list_tiles * LANES - 1)
        return list_sm[g >> 7, g & (LANES - 1)]

    def chosen(g):
        cell = lax.rem(entry(g), cells)
        place_row = jnp.broadcast_to(place_ref[pl.ds(cell, 1), :], (SUB, slots))
        return cell, place_row == sub_row + g * SUB

    def gather(body):
        for k in range(GROUPS):
            cell, mask = chosen(body * GROUPS + k)
            for f in range(3):
                value = jnp.where(mask, rel_ref[own, f, pl.ds(cell, 1), :], 0.0)
                value = sum(value[:, t * LANES:(t + 1) * LANES] for t in range(tiles))
                target_ref[3 * k + f] = jnp.broadcast_to(jnp.sum(value, axis=1, keepdims=True), (SUB, LANES))

    def scatter(body):
        for k in range(GROUPS):
            cell, mask = chosen(body * GROUPS + k)
            total = jnp.sum(acc_ref[k], axis=1, keepdims=True)
            sums_ref[cell] = sums_ref[cell] + jnp.where(mask, total, 0.0)

    def work(g):
        code = entry(g)
        octant = code // cells
        cell = code - octant * cells
        rod = octant >> 1
        side = octant & 1
        other = lax.rem(cell + 2 * side - 1 + cells, cells)
        return rod, cell, other, jnp.where(side == 1, -4.0, 4.0)

    def part(rod, cell, at, ty, tx, tz, acc):
        y, x, z, mass = (source_ref[(4 * rod + f) * wide + at, pl.ds(cell, SUB, stride=0)] for f in range(4))
        dy, dx, dz = y - ty, x - tx, z - tz
        squared = jnp.maximum(dy * dy + dx * dx + dz * dz, 1e-30)
        q = squared * lax.rsqrt(squared)
        outer = jnp.maximum(2.0 - q, 0.0)
        inner = jnp.maximum(1.0 - q, 0.0)
        value = outer * outer * outer - 4.0 * (inner * inner * inner)
        return acc + mass * value

    near = wide // 2

    def compute(body, begin, finish, fresh):
        for k in range(GROUPS):
            rod, cell, other, offset = work(body * GROUPS + k)
            ty, tx, tz = target_ref[3 * k], target_ref[3 * k + 1], target_ref[3 * k + 2]
            moved = tx + offset
            acc = jnp.zeros((SUB, LANES), f32) if fresh else acc_ref[k]
            for at in range(begin, finish):
                acc = part(rod, cell, at, ty, tx, tz, acc)
                acc = part(rod, other, at, ty, moved, tz, acc)
            acc_ref[k] = acc

    sums_ref[...] = jnp.zeros(sums_ref.shape, f32)
    acc_ref[...] = jnp.zeros(acc_ref.shape, f32)
    bodies = (list_sm[list_tiles, 0] + (GROUPS - 1)) // GROUPS
    gather(0)

    def body_step(body, carry):
        most = 0
        for k in range(GROUPS):
            rod, cell, other, _ = work(body * GROUPS + k)
            most = jnp.maximum(most, list_sm[list_tiles + 1, rod * cells + cell])
            most = jnp.maximum(most, list_sm[list_tiles + 1, rod * cells + other])
        scatter(body - 1)

        compute(body, 0, near, True)

        @pl.when(most > near)
        def _():
            compute(body, near, wide, False)

        gather(body + 1)
        return carry

    lax.fori_loop(0, bodies, body_step, 0)
    scatter(bodies - 1)
    for cell in range(cells):
        total = jnp.sum(sums_ref[cell], axis=0, keepdims=True) * (16.0 / 3.141592653589793)
        for t in range(tiles):
            out_ref[cell * tiles + t:cell * tiles + t + 1, :] = total[:, t * LANES:(t + 1) * LANES]


def shards(positions, masses, counts, shear_offset):
    cells_y, cells, cells_z, slots = masses.shape
    assert cells_y == 1 and cells_z == 1 and slots % LANES == 0
    tiles = slots // LANES
    rows = cells * tiles
    slot = lax.broadcasted_iota(jnp.int32, (rows, LANES), 1)
    slot = slot + LANES * lax.rem(lax.broadcasted_iota(jnp.int32, (rows, LANES), 0), tiles)
    held = jnp.repeat(counts.reshape(cells), tiles)[:, None]
    weight = jnp.where(slot < held, masses.reshape(rows, LANES), jnp.float32(0.0))
    data = jnp.concatenate([positions.reshape(3, rows, LANES), weight[None]], 0)
    padded = halo(data)
    offset = shear_offset[0]
    shear_index = lax.axis_index("shear")
    cycle = lax.axis_size("shear")
    low = jnp.where(shear_index == 0, offset, 0) % cells
    high = jnp.where(shear_index == cycle - 1, -offset, 0) % cells
    rolls = jnp.stack([low, high]).astype(jnp.int32)

    octants = 2 * len(RODS)
    most_groups = cells * (slots // SUB + octants - 1)
    list_tiles = -(-(most_groups + GROUPS) // LANES)
    wide = 4 * slots
    smem = pl.BlockSpec(memory_space=pltpu.SMEM)
    vmem = pl.BlockSpec(memory_space=pltpu.VMEM)
    density = pl.pallas_call(
        functools.partial(density_kernel, cells),
        out_shape=jax.ShapeDtypeStruct((rows, LANES), jnp.float32),
        in_specs=[smem, vmem],
        out_specs=vmem,
        scratch_shapes=[
            pltpu.VMEM((9, 4, cells, slots), jnp.float32),
            pltpu.VMEM((4 * len(RODS) * wide // LANES, cells, LANES), jnp.float32),
            pltpu.VMEM((cells, slots), jnp.int32),
            pltpu.VMEM((3 * GROUPS, SUB, LANES), jnp.float32),
            pltpu.VMEM((GROUPS, SUB, LANES), jnp.float32),
            pltpu.VMEM((cells, SUB, slots), jnp.float32),
            pltpu.VMEM((list_tiles + 2, LANES), jnp.int32),
            pltpu.SMEM((list_tiles + 2, LANES), jnp.int32),
            pltpu.SemaphoreType.DMA,
        ],
        compiler_params=pltpu.CompilerParams(vmem_limit_bytes=56 * 1024 * 1024),
        name="density",
    )(rolls, padded)
    return density.reshape(masses.shape)


def solution(mesh):
    in_specs = (
        P(None, "shear", None, "cross", None),
        P("shear", None, "cross", None),
        P("shear", None, "cross"),
        P(),
    )
    out_specs = P("shear", None, "cross", None)
    return jax.shard_map(shards, mesh=mesh, in_specs=in_specs, out_specs=out_specs, check_vma=False)
```

```python
import functools
import jax
import jax.numpy as jnp
from jax import lax
from jax.experimental import pallas as pl
from jax.experimental.pallas import tpu as pltpu
from jax.sharding import PartitionSpec as P

LANES = 128
SUB = 8
GROUPS = 8
RODS = ((0, 0), (0, 1), (1, 0), (1, 1))


def halo_kernel(data_ref, out_ref, send_sems, recv_sems, local_sem):
    shear, cross = lax.axis_index("shear"), lax.axis_index("cross")
    rows, planes = lax.axis_size("shear"), lax.axis_size("cross")
    mesh_ids = pl.DeviceIdType.MESH
    along_y = [(lax.rem(shear + rows - step, rows), cross) for step in (-1, 1)]
    along_z = [(shear, lax.rem(cross + planes - step, planes)) for step in (-1, 1)]
    barrier = pltpu.get_barrier_semaphore()
    for device in along_y + along_z:
        pl.semaphore_signal(barrier, inc=1, device_id=device, device_id_type=mesh_ids)
    own = pltpu.make_async_copy(data_ref, out_ref.at[1, 1], local_sem)
    own.start()
    pl.semaphore_wait(barrier, 4)

    def sent(source, y, z, device):
        slot = 3 * y + z
        copy = pltpu.make_async_remote_copy(
            src_ref=source,
            dst_ref=out_ref.at[y, z],
            send_sem=send_sems.at[slot],
            recv_sem=recv_sems.at[slot],
            device_id=device,
            device_id_type=mesh_ids,
        )
        copy.start()
        return copy

    rows_sent = [sent(data_ref, y, 1, along_y[k]) for k, y in enumerate((0, 2))]
    planes_sent = [sent(data_ref, 1, z, along_z[k]) for k, z in enumerate((0, 2))]
    for k, y in enumerate((0, 2)):
        rows_sent[k].wait_recv()
        for j, z in enumerate((0, 2)):
            planes_sent.append(sent(out_ref.at[y, 1], y, z, along_z[j]))
    for copy in rows_sent:
        copy.wait_send()
    for copy in planes_sent:
        copy.wait()
    own.wait()


def halo(data):
    vmem = pl.BlockSpec(memory_space=pltpu.VMEM)
    return pl.pallas_call(
        halo_kernel,
        out_shape=jax.ShapeDtypeStruct((3, 3) + data.shape, data.dtype),
        in_specs=[vmem],
        out_specs=vmem,
        scratch_shapes=[
            pltpu.SemaphoreType.DMA((9,)),
            pltpu.SemaphoreType.DMA((9,)),
            pltpu.SemaphoreType.DMA,
        ],
        compiler_params=pltpu.CompilerParams(collective_id=0, has_side_effects=True),
        name="halo",
    )(data)


def density_kernel(
    cells, roll_ref, data_ref, out_ref,
    rel_ref, source_ref, place_ref, target_ref, acc_ref, sums_ref, list_ref, list_sm, list_sem,
):
    f32, i32 = jnp.float32, jnp.int32
    tiles = data_ref.shape[3] // cells
    slots = tiles * LANES
    wide = 4 * tiles
    list_tiles = list_ref.shape[0] - 1
    near = wide // 2
    half = 0.5

    masks = {}
    for sy in (-1, 0, 1):
        for sz in (-1, 0, 1):
            relation = 3 * (sy + 1) + sz + 1
            parts = []
            for k in range(4):
                value = jnp.concatenate(
                    [data_ref[sy + 1, sz + 1, k, pl.ds(t, cells, stride=tiles), :] for t in range(tiles)], axis=1
                )
                if sy != 0:
                    value = pltpu.roll(value, roll_ref[(sy + 1) // 2], 0)
                parts.append(value)
            y, x, z, mass = parts
            keep = mass > 0.0
            if sy == -1:
                keep = keep & (y >= half)
            elif sy == 1:
                keep = keep & (y <= half)
            if sz == -1:
                keep = keep & (z >= half)
            elif sz == 1:
                keep = keep & (z <= half)
            masks[sy, sz] = keep
            rel_ref[relation, 0] = 4.0 * (y + (sy - half))
            rel_ref[relation, 1] = 4.0 * (x - half)
            rel_ref[relation, 2] = 4.0 * (z + (sz - half))
            rel_ref[relation, 3] = mass
            if sy == 0 and sz == 0:
                own_y, own_x, own_z, own_valid = y, x, z, keep

    octants = []
    for ry, rz in RODS:
        inside = own_valid & ((own_y >= half) if ry else (own_y < half))
        inside = inside & ((own_z >= half) if rz else (own_z < half))
        octants.append(inside & (own_x < half))
        octants.append(inside & (own_x >= half))

    relations = [(sy, sz) for sy in (-1, 0, 1) for sz in (-1, 0, 1)]
    stacked = jnp.concatenate(
        [jnp.where(masks[r], 1.0, 0.0) for r in relations] + [jnp.where(m, 1.0, 0.0) for m in octants], axis=0
    ).astype(jnp.bfloat16)
    row = lax.broadcasted_iota(i32, (slots, slots + LANES), 0)
    col = lax.broadcasted_iota(i32, (slots, slots + LANES), 1)
    triangle = jnp.where((row <= col) | (col >= slots), 1.0, 0.0).astype(jnp.bfloat16)
    ranks = jnp.dot(stacked, triangle, preferred_element_type=f32).astype(i32)

    first = len(relations) * cells
    totals = ranks[first:, slots:]
    groups = (totals + (SUB - 1)) >> 3
    n_oct = len(octants) * cells
    lower = jnp.where(
        lax.broadcasted_iota(i32, (n_oct, n_oct), 1) < lax.broadcasted_iota(i32, (n_oct, n_oct), 0), 1.0, 0.0
    ).astype(jnp.bfloat16)
    base = jnp.dot(lower, groups.astype(f32).astype(jnp.bfloat16), preferred_element_type=f32).astype(i32)
    end = base + groups
    place = jnp.full((cells, slots), -1, i32)
    for o, inside in enumerate(octants):
        begin = base[o * cells:(o + 1) * cells]
        begin = jnp.concatenate([begin] * tiles, axis=1)
        rank = ranks[first + o * cells:first + (o + 1) * cells, :slots]
        place = jnp.where(inside, SUB * begin + rank - 1, place)
    place_ref[...] = place
    cell_row = lax.broadcasted_iota(i32, (cells, LANES), 0)
    rods, words = [], []
    for r, (ry, rz) in enumerate(RODS):
        segments = [(0, 0), (2 * ry - 1, 0), (0, 2 * rz - 1), (2 * ry - 1, 2 * rz - 1)]
        starts, start = [], jnp.zeros((cells, LANES), i32)
        for sy, sz in segments:
            at = (3 * (sy + 1) + sz + 1) * cells
            starts.append(start)
            start = start + ranks[at:at + cells, slots:]
        rods.append((segments, starts, start))
        for side in range(2):
            other = pltpu.roll(cell_row, cells - 1 if side else 1, 0)
            far = jnp.maximum(start, pltpu.roll(start, cells - 1 if side else 1, 0)) > near * LANES
            word = (r * cells + cell_row) + ((r * cells + other) << 7) + (cell_row << 14)
            words.append(word + (side << 19) + jnp.where(far, 1 << 20, 0))
    word = jnp.concatenate(words, axis=0)
    change = pltpu.roll(word, n_oct - 1, 0) - word
    change = jnp.where(lax.broadcasted_iota(i32, (n_oct, LANES), 0) < n_oct - 1, change, 0).astype(f32)
    lane = lax.broadcasted_iota(i32, (n_oct, LANES), 1)
    for j in range(list_tiles):
        passed = jnp.where(end <= lane + (j * LANES - GROUPS), change, 0.0)
        list_ref[j:j + 1, :] = word[:1] + jnp.sum(passed, axis=0, keepdims=True).astype(i32)
    list_ref[list_tiles:list_tiles + 1, :] = end[n_oct - 1:n_oct]

    lane8 = lax.broadcasted_iota(i32, (SUB, LANES), 1)
    copy = None
    for r, (segments, starts, total) in enumerate(rods):
        for top in range(0, cells, SUB):
            rows = slice(top, top + SUB)
            held = slice(r * cells + top, r * cells + top + SUB)
            arrays = [[] for _ in range(4)]
            moves = []
            for k, (sy, sz) in enumerate(segments):
                relation = 3 * (sy + 1) + sz + 1
                for t in range(tiles):
                    lanes = slice(t * LANES, (t + 1) * LANES)
                    for f in range(4):
                        arrays[f].append(rel_ref[relation, f, rows, lanes])
                    if k == 0:
                        moves.append(jnp.zeros((SUB, LANES), i32))
                    else:
                        at = relation * cells + top
                        shift = (k * slots + t * LANES + 1) + lane8 - starts[k][rows] - ranks[at:at + SUB, lanes]
                        moves.append(jnp.where(masks[sy, sz][rows, lanes], shift, 0))
            step = 1
            while step < wide * LANES:
                if step < LANES:
                    inner = lane8 < LANES - step

                    def shifted(values, edge=None):
                        turned = [pltpu.roll(v, LANES - step, 1) for v in values]
                        last = turned[-1] if edge is None else jnp.where(inner, turned[-1], edge)
                        return [jnp.where(inner, a, b) for a, b in zip(turned, turned[1:])] + [last]

                    moved = [shifted(a) for a in arrays]
                    moved_d = shifted(moves, 0)
                    reach = wide
                else:
                    q = step // LANES
                    moved = [a[q:] for a in arrays]
                    moved_d = moves[q:]
                    reach = wide - q
                leaving = [(d & step) != 0 for d in moves]
                coming = [(d & step) != 0 for d in moved_d]
                arrays = [
                    [jnp.where(coming[j], m[j], a[j]) if j < reach else a[j] for j in range(wide)]
                    for m, a in zip(moved, arrays)
                ]
                kept = [jnp.where(leaving[j], 0, moves[j]) for j in range(wide)]
                moves = [jnp.where(coming[j], moved_d[j], kept[j]) if j < reach else kept[j] for j in range(wide)]
                step *= 2
            for j in range(wide):
                for f in range(3):
                    source_ref[f * wide + j, held] = arrays[f][j]
                source_ref[3 * wide + j, held] = jnp.where(
                    lane8 + j * LANES < total[rows], arrays[3][j], 0.0
                )
        if copy is None:
            copy = pltpu.make_async_copy(list_ref, list_sm, list_sem)
            copy.start()
    copy.wait()

    sub_row = lax.broadcasted_iota(i32, (SUB, slots), 0)
    own = 4

    def entries(body):
        at = (body + 1) * GROUPS
        line, at = at >> 7, at & (LANES - 1)
        return [list_sm[line, at + k] for k in range(GROUPS)]

    def chosen(word, g):
        cell = (word >> 14) & 31
        place_row = jnp.broadcast_to(place_ref[pl.ds(cell, 1), :], (SUB, slots))
        return cell, place_row == sub_row + g * SUB

    def gather(body):
        buffer = (body & 1) * (3 * GROUPS)
        for k, word in enumerate(entries(body)):
            cell, mask = chosen(word, body * GROUPS + k)
            for f in range(3):
                value = jnp.where(mask, rel_ref[own, f, pl.ds(cell, 1), :], 0.0)
                value = sum(value[:, t * LANES:(t + 1) * LANES] for t in range(tiles))
                target_ref[buffer + 3 * k + f] = jnp.broadcast_to(jnp.sum(value, axis=1, keepdims=True), (SUB, LANES))

    def scatter(body):
        for k, word in enumerate(entries(body)):
            cell, mask = chosen(word, body * GROUPS + k)
            total = jnp.sum(acc_ref[k], axis=1, keepdims=True)
            sums_ref[cell] = sums_ref[cell] + jnp.where(mask, total, 0.0)

    def part(line, at, ty, tx, tz, acc):
        y, x, z, mass = (source_ref[f * wide + at, pl.ds(line, SUB, stride=0)] for f in range(4))
        dy, dx, dz = y - ty, x - tx, z - tz
        squared = jnp.maximum(dy * dy + dx * dx + dz * dz, 1e-30)
        q = squared * lax.rsqrt(squared)
        outer = jnp.maximum(2.0 - q, 0.0)
        inner = jnp.maximum(1.0 - q, 0.0)
        value = outer * outer * outer - 4.0 * (inner * inner * inner)
        return acc + mass * value

    def compute(body, words, begin, finish, fresh):
        buffer = (body & 1) * (3 * GROUPS)
        for k, word in enumerate(words):
            line, other = word & 127, (word >> 7) & 127
            offset = jnp.where((word & (1 << 19)) != 0, -4.0, 4.0)
            ty, tx, tz = (target_ref[buffer + 3 * k + f] for f in range(3))
            moved = tx + offset
            acc = jnp.zeros((SUB, LANES), f32) if fresh else acc_ref[k]
            for at in range(begin, finish):
                acc = part(line, at, ty, tx, tz, acc)
                acc = part(other, at, ty, moved, tz, acc)
            acc_ref[k] = acc

    sums_ref[...] = jnp.zeros(sums_ref.shape, f32)
    acc_ref[...] = jnp.zeros(acc_ref.shape, f32)
    bodies = (list_sm[list_tiles, 0] + (GROUPS - 1)) // GROUPS
    gather(0)

    def body_step(body, carry):
        words = entries(body)
        scatter(body - 1)
        compute(body, words, 0, near, True)
        gather(body + 1)
        flags = words[0]
        for word in words[1:]:
            flags = flags | word

        @pl.when((flags & (1 << 20)) != 0)
        def _():
            compute(body, words, near, wide, False)

        return carry

    lax.fori_loop(0, bodies, body_step, 0)
    scatter(bodies - 1)
    for cell in range(cells):
        total = jnp.sum(sums_ref[cell], axis=0, keepdims=True) * (16.0 / 3.141592653589793)
        for t in range(tiles):
            out_ref[cell * tiles + t:cell * tiles + t + 1, :] = total[:, t * LANES:(t + 1) * LANES]


def shards(positions, masses, counts, shear_offset):
    cells_y, cells, cells_z, slots = masses.shape
    assert cells_y == 1 and cells_z == 1 and slots % LANES == 0
    tiles = slots // LANES
    rows = cells * tiles
    slot = lax.broadcasted_iota(jnp.int32, (rows, LANES), 1)
    slot = slot + LANES * lax.rem(lax.broadcasted_iota(jnp.int32, (rows, LANES), 0), tiles)
    held = jnp.repeat(counts.reshape(cells), tiles)[:, None]
    weight = jnp.where(slot < held, masses.reshape(rows, LANES), jnp.float32(0.0))
    data = jnp.concatenate([positions.reshape(3, rows, LANES), weight[None]], 0)
    padded = halo(data)
    offset = shear_offset[0]
    shear_index = lax.axis_index("shear")
    cycle = lax.axis_size("shear")
    low = jnp.where(shear_index == 0, offset, 0) % cells
    high = jnp.where(shear_index == cycle - 1, -offset, 0) % cells
    rolls = jnp.stack([low, high]).astype(jnp.int32)

    octants = 2 * len(RODS)
    most_groups = cells * (slots // SUB + octants - 1)
    list_tiles = -(-(most_groups + 3 * GROUPS) // LANES)
    wide = 4 * slots
    smem = pl.BlockSpec(memory_space=pltpu.SMEM)
    vmem = pl.BlockSpec(memory_space=pltpu.VMEM)
    density = pl.pallas_call(
        functools.partial(density_kernel, cells),
        out_shape=jax.ShapeDtypeStruct((rows, LANES), jnp.float32),
        in_specs=[smem, vmem],
        out_specs=vmem,
        scratch_shapes=[
            pltpu.VMEM((9, 4, cells, slots), jnp.float32),
            pltpu.VMEM((4 * wide // LANES, len(RODS) * cells, LANES), jnp.float32),
            pltpu.VMEM((cells, slots), jnp.int32),
            pltpu.VMEM((6 * GROUPS, SUB, LANES), jnp.float32),
            pltpu.VMEM((GROUPS, SUB, LANES), jnp.float32),
            pltpu.VMEM((cells, SUB, slots), jnp.float32),
            pltpu.VMEM((list_tiles + 1, LANES), jnp.int32),
            pltpu.SMEM((list_tiles + 1, LANES), jnp.int32),
            pltpu.SemaphoreType.DMA,
        ],
        compiler_params=pltpu.CompilerParams(vmem_limit_bytes=56 * 1024 * 1024),
        name="density",
    )(rolls, padded)
    return density.reshape(masses.shape)


def solution(mesh):
    in_specs = (
        P(None, "shear", None, "cross", None),
        P("shear", None, "cross", None),
        P("shear", None, "cross"),
        P(),
    )
    out_specs = P("shear", None, "cross", None)
    return jax.shard_map(shards, mesh=mesh, in_specs=in_specs, out_specs=out_specs, check_vma=False)
```

```python
import functools
import jax
import jax.numpy as jnp
from jax import lax
from jax.experimental import pallas as pl
from jax.experimental.pallas import tpu as pltpu
from jax.sharding import PartitionSpec as P

LANES = 128
SUB = 8
GROUPS = 8
RODS = ((0, 0), (0, 1), (1, 0), (1, 1))


def halo_kernel(data_ref, out_ref, send_sems, recv_sems, local_sem):
    shear, cross = lax.axis_index("shear"), lax.axis_index("cross")
    rows, planes = lax.axis_size("shear"), lax.axis_size("cross")
    mesh_ids = pl.DeviceIdType.MESH
    along_y = [(lax.rem(shear + rows - step, rows), cross) for step in (-1, 1)]
    along_z = [(shear, lax.rem(cross + planes - step, planes)) for step in (-1, 1)]
    barrier = pltpu.get_barrier_semaphore()
    for device in along_y + along_z:
        pl.semaphore_signal(barrier, inc=1, device_id=device, device_id_type=mesh_ids)
    own = pltpu.make_async_copy(data_ref, out_ref.at[1, 1], local_sem)
    own.start()
    pl.semaphore_wait(barrier, 4)

    def sent(source, y, z, device):
        slot = 3 * y + z
        copy = pltpu.make_async_remote_copy(
            src_ref=source,
            dst_ref=out_ref.at[y, z],
            send_sem=send_sems.at[slot],
            recv_sem=recv_sems.at[slot],
            device_id=device,
            device_id_type=mesh_ids,
        )
        copy.start()
        return copy

    rows_sent = [sent(data_ref, y, 1, along_y[k]) for k, y in enumerate((0, 2))]
    planes_sent = [sent(data_ref, 1, z, along_z[k]) for k, z in enumerate((0, 2))]
    for k, y in enumerate((0, 2)):
        rows_sent[k].wait_recv()
        for j, z in enumerate((0, 2)):
            planes_sent.append(sent(out_ref.at[y, 1], y, z, along_z[j]))
    for copy in rows_sent:
        copy.wait_send()
    for copy in planes_sent:
        copy.wait()
    own.wait()


def halo(data):
    vmem = pl.BlockSpec(memory_space=pltpu.VMEM)
    return pl.pallas_call(
        halo_kernel,
        out_shape=jax.ShapeDtypeStruct((3, 3) + data.shape, data.dtype),
        in_specs=[vmem],
        out_specs=vmem,
        scratch_shapes=[
            pltpu.SemaphoreType.DMA((9,)),
            pltpu.SemaphoreType.DMA((9,)),
            pltpu.SemaphoreType.DMA,
        ],
        compiler_params=pltpu.CompilerParams(
            collective_id=0, has_side_effects=True, vmem_limit_bytes=4 * 1024 * 1024
        ),
        name="halo",
    )(data)


def density_kernel(
    cells, roll_ref, data_ref, out_ref,
    rel_ref, source_ref, move_ref, total_ref, place_ref, target_ref, acc_ref, sums_ref, list_ref, list_sm, list_sem,
):
    f32, i32 = jnp.float32, jnp.int32
    tiles = data_ref.shape[3] // cells
    slots = tiles * LANES
    wide = 4 * tiles
    list_tiles = list_ref.shape[0] - 1
    near = wide // 2
    half = 0.5

    masks = {}
    for sy in (-1, 0, 1):
        for sz in (-1, 0, 1):
            relation = 3 * (sy + 1) + sz + 1
            parts = []
            for k in range(4):
                value = jnp.concatenate(
                    [data_ref[sy + 1, sz + 1, k, pl.ds(t, cells, stride=tiles), :] for t in range(tiles)], axis=1
                )
                if sy != 0:
                    value = pltpu.roll(value, roll_ref[(sy + 1) // 2], 0)
                parts.append(value)
            y, x, z, mass = parts
            keep = mass > 0.0
            if sy == -1:
                keep = keep & (y >= half)
            elif sy == 1:
                keep = keep & (y <= half)
            if sz == -1:
                keep = keep & (z >= half)
            elif sz == 1:
                keep = keep & (z <= half)
            masks[sy, sz] = keep
            rel_ref[relation, 0] = 4.0 * (y + (sy - half))
            rel_ref[relation, 1] = 4.0 * (x - half)
            rel_ref[relation, 2] = 4.0 * (z + (sz - half))
            rel_ref[relation, 3] = mass
            if sy == 0 and sz == 0:
                own_y, own_x, own_z, own_valid = y, x, z, keep

    octants = []
    for ry, rz in RODS:
        inside = own_valid & ((own_y >= half) if ry else (own_y < half))
        inside = inside & ((own_z >= half) if rz else (own_z < half))
        octants.append(inside & (own_x < half))
        octants.append(inside & (own_x >= half))

    relations = [(sy, sz) for sy in (-1, 0, 1) for sz in (-1, 0, 1)]
    stacked = jnp.concatenate(
        [jnp.where(masks[r], 1.0, 0.0) for r in relations] + [jnp.where(m, 1.0, 0.0) for m in octants], axis=0
    ).astype(jnp.bfloat16)
    row = lax.broadcasted_iota(i32, (slots, slots + LANES), 0)
    col = lax.broadcasted_iota(i32, (slots, slots + LANES), 1)
    triangle = jnp.where((row <= col) | (col >= slots), 1.0, 0.0).astype(jnp.bfloat16)
    ranks = jnp.dot(stacked, triangle, preferred_element_type=f32).astype(i32)

    first = len(relations) * cells
    totals = ranks[first:, slots:]
    groups = (totals + (SUB - 1)) >> 3
    n_oct = len(octants) * cells
    lower = jnp.where(
        lax.broadcasted_iota(i32, (n_oct, n_oct), 1) < lax.broadcasted_iota(i32, (n_oct, n_oct), 0), 1.0, 0.0
    ).astype(jnp.bfloat16)
    base = jnp.dot(lower, groups.astype(f32).astype(jnp.bfloat16), preferred_element_type=f32).astype(i32)
    end = base + groups
    place = jnp.full((cells, slots), -1, i32)
    for o, inside in enumerate(octants):
        begin = base[o * cells:(o + 1) * cells]
        begin = jnp.concatenate([begin] * tiles, axis=1)
        rank = ranks[first + o * cells:first + (o + 1) * cells, :slots]
        place = jnp.where(inside, SUB * begin + rank - 1, place)
    place_ref[...] = place
    cell_row = lax.broadcasted_iota(i32, (cells, LANES), 0)
    rods, words = [], []
    for r, (ry, rz) in enumerate(RODS):
        segments = [(0, 0), (2 * ry - 1, 0), (0, 2 * rz - 1), (2 * ry - 1, 2 * rz - 1)]
        starts, start = [], jnp.zeros((cells, LANES), i32)
        for sy, sz in segments:
            at = (3 * (sy + 1) + sz + 1) * cells
            starts.append(start)
            start = start + ranks[at:at + cells, slots:]
        rods.append((segments, starts, start))
        for side in range(2):
            other = pltpu.roll(cell_row, cells - 1 if side else 1, 0)
            far = jnp.maximum(start, pltpu.roll(start, cells - 1 if side else 1, 0)) > near * LANES
            word = (r * cells + cell_row) + ((r * cells + other) << 7) + (cell_row << 14)
            words.append(word + (side << 19) + jnp.where(far, 1 << 20, 0))
    word = jnp.concatenate(words, axis=0)
    change = pltpu.roll(word, n_oct - 1, 0) - word
    change = jnp.where(lax.broadcasted_iota(i32, (n_oct, LANES), 0) < n_oct - 1, change, 0).astype(f32)
    lane = lax.broadcasted_iota(i32, (n_oct, LANES), 1)
    for j in range(list_tiles):
        passed = jnp.where(end <= lane + (j * LANES - GROUPS), change, 0.0)
        list_ref[j:j + 1, :] = word[:1] + jnp.sum(passed, axis=0, keepdims=True).astype(i32)
    list_ref[list_tiles:list_tiles + 1, :] = end[n_oct - 1:n_oct]

    copy = pltpu.make_async_copy(list_ref, list_sm, list_sem)
    lane = lax.broadcasted_iota(i32, (cells, LANES), 1)
    for r, (segments, starts, total) in enumerate(rods):
        held = slice(r * cells, (r + 1) * cells)
        total_ref[held] = total
        for k, (sy, sz) in enumerate(segments):
            at = (3 * (sy + 1) + sz + 1) * cells
            for t in range(tiles):
                lanes = slice(t * LANES, (t + 1) * LANES)
                word = lane << 10
                if k > 0:
                    shift = (k * slots + t * LANES + 1) + lane - starts[k] - ranks[at:at + cells, lanes]
                    word = word + jnp.where(masks[sy, sz][:, lanes], shift, 0)
                move_ref[k * tiles + t, held] = word
    copy.start()

    lane8 = lax.broadcasted_iota(i32, (SUB, LANES), 1)
    blocks = len(RODS) * cells // SUB

    def stage(k, carry):
        step = 1 << k
        inner = lane8 < LANES - step
        for block in range(blocks):
            held = slice(block * SUB, (block + 1) * SUB)
            words = [move_ref[j, held] for j in range(tiles - 1, wide)]
            turned = [pltpu.roll(w, LANES - step, 1) for w in words] + [jnp.zeros_like(lane8)]
            for j, word in enumerate(words):
                coming = jnp.where(inner, turned[j], turned[j + 1])
                word = jnp.where((word & step) != 0, 0, word)
                move_ref[j + tiles - 1, held] = jnp.where((coming & step) != 0, coming, word)
        return carry

    lax.fori_loop(0, LANES.bit_length() - 1, stage, 0)

    def settle(block, carry):
        rod = block // (cells // SUB)
        top = pl.multiple_of((block - rod * (cells // SUB)) * SUB, SUB)
        held = pl.ds(pl.multiple_of(block * SUB, SUB), SUB)
        ry, rz = 2 * (rod >> 1), 2 * (rod & 1)
        segments = [4, 3 * ry + 1, 3 + rz, 3 * ry + rz]
        words = [move_ref[j, held] for j in range(wide)]
        origin = [w >> 10 for w in words]
        data = []
        for f in range(4):
            raw = [
                rel_ref[segments[j // tiles], f, pl.ds(top, SUB), (j % tiles) * LANES:(j % tiles + 1) * LANES]
                for j in range(wide)
            ]
            moved = []
            for j in range(wide):
                here = raw[j] if j < tiles else jnp.take_along_axis(raw[j], origin[j], axis=1, mode="promise_in_bounds")
                if tiles - 1 <= j < wide - 1:
                    after = jnp.take_along_axis(raw[j + 1], origin[j], axis=1, mode="promise_in_bounds")
                    here = jnp.where(origin[j] >= lane8, here, after)
                moved.append(here)
            data.append(moved)
        step = LANES
        while step < wide * LANES:
            q = step // LANES
            coming = [(w & step) != 0 for w in words[q:]]
            leaving = [(w & step) != 0 for w in words]
            kept = [jnp.where(leaving[j], 0, words[j]) for j in range(wide)]
            words = [jnp.where(coming[j], words[j + q], kept[j]) for j in range(wide - q)] + kept[wide - q:]
            data = [[jnp.where(coming[j], a[j + q], a[j]) for j in range(wide - q)] + a[wide - q:] for a in data]
            step *= 2
        total = total_ref[held]
        for j in range(wide):
            for f in range(3):
                source_ref[f * wide + j, held] = data[f][j]
            source_ref[3 * wide + j, held] = jnp.where(lane8 + j * LANES < total, data[3][j], 0.0)
        return carry

    lax.fori_loop(0, blocks, settle, 0)
    copy.wait()

    sub_row = lax.broadcasted_iota(i32, (SUB, slots), 0)
    own = 4

    def entries(body):
        at = (body + 1) * GROUPS
        line, at = at >> 7, at & (LANES - 1)
        return [list_sm[line, at + k] for k in range(GROUPS)]

    def chosen(word, g):
        cell = (word >> 14) & 31
        place_row = jnp.broadcast_to(place_ref[pl.ds(cell, 1), :], (SUB, slots))
        return cell, place_row == sub_row + g * SUB

    def gather(body):
        buffer = (body & 1) * (3 * GROUPS)
        for k, word in enumerate(entries(body)):
            cell, mask = chosen(word, body * GROUPS + k)
            for f in range(3):
                value = jnp.where(mask, rel_ref[own, f, pl.ds(cell, 1), :], 0.0)
                value = sum(value[:, t * LANES:(t + 1) * LANES] for t in range(tiles))
                target_ref[buffer + 3 * k + f] = jnp.broadcast_to(jnp.sum(value, axis=1, keepdims=True), (SUB, LANES))

    def scatter(body):
        for k, word in enumerate(entries(body)):
            cell, mask = chosen(word, body * GROUPS + k)
            total = jnp.sum(acc_ref[k], axis=1, keepdims=True)
            sums_ref[cell] = sums_ref[cell] + jnp.where(mask, total, 0.0)

    def part(line, at, ty, tx, tz, acc):
        y, x, z, mass = (source_ref[f * wide + at, pl.ds(line, SUB, stride=0)] for f in range(4))
        dy, dx, dz = y - ty, x - tx, z - tz
        squared = jnp.maximum(dy * dy + dx * dx + dz * dz, 1e-30)
        q = squared * lax.rsqrt(squared)
        outer = jnp.maximum(2.0 - q, 0.0)
        inner = jnp.maximum(1.0 - q, 0.0)
        value = outer * outer * outer - 4.0 * (inner * inner * inner)
        return acc + mass * value

    def compute(body, words, begin, finish, fresh):
        buffer = (body & 1) * (3 * GROUPS)
        for k, word in enumerate(words):
            line, other = word & 127, (word >> 7) & 127
            offset = jnp.where((word & (1 << 19)) != 0, -4.0, 4.0)
            ty, tx, tz = (target_ref[buffer + 3 * k + f] for f in range(3))
            moved = tx + offset
            acc = jnp.zeros((SUB, LANES), f32) if fresh else acc_ref[k]
            for at in range(begin, finish):
                acc = part(line, at, ty, tx, tz, acc)
                acc = part(other, at, ty, moved, tz, acc)
            acc_ref[k] = acc

    sums_ref[...] = jnp.zeros(sums_ref.shape, f32)
    acc_ref[...] = jnp.zeros(acc_ref.shape, f32)
    bodies = (list_sm[list_tiles, 0] + (GROUPS - 1)) // GROUPS
    gather(0)

    def body_step(body, carry):
        words = entries(body)
        scatter(body - 1)
        compute(body, words, 0, near, True)
        gather(body + 1)
        flags = words[0]
        for word in words[1:]:
            flags = flags | word

        @pl.when((flags & (1 << 20)) != 0)
        def _():
            compute(body, words, near, wide, False)

        return carry

    lax.fori_loop(0, bodies, body_step, 0)
    scatter(bodies - 1)
    for cell in range(cells):
        total = jnp.sum(sums_ref[cell], axis=0, keepdims=True) * (16.0 / 3.141592653589793)
        for t in range(tiles):
            out_ref[cell * tiles + t:cell * tiles + t + 1, :] = total[:, t * LANES:(t + 1) * LANES]


def shards(positions, masses, counts, shear_offset):
    cells_y, cells, cells_z, slots = masses.shape
    assert cells_y == 1 and cells_z == 1 and slots % LANES == 0
    tiles = slots // LANES
    rows = cells * tiles
    slot = lax.broadcasted_iota(jnp.int32, (rows, LANES), 1)
    slot = slot + LANES * lax.rem(lax.broadcasted_iota(jnp.int32, (rows, LANES), 0), tiles)
    held = jnp.repeat(counts.reshape(cells), tiles)[:, None]
    weight = jnp.where(slot < held, masses.reshape(rows, LANES), jnp.float32(0.0))
    data = jnp.concatenate([positions.reshape(3, rows, LANES), weight[None]], 0)
    padded = halo(data)
    offset = shear_offset[0]
    shear_index = lax.axis_index("shear")
    cycle = lax.axis_size("shear")
    low = jnp.where(shear_index == 0, offset, 0) % cells
    high = jnp.where(shear_index == cycle - 1, -offset, 0) % cells
    rolls = jnp.stack([low, high]).astype(jnp.int32)

    octants = 2 * len(RODS)
    most_groups = cells * (slots // SUB + octants - 1)
    list_tiles = -(-(most_groups + 3 * GROUPS) // LANES)
    wide = 4 * slots
    smem = pl.BlockSpec(memory_space=pltpu.SMEM)
    vmem = pl.BlockSpec(memory_space=pltpu.VMEM)
    density = pl.pallas_call(
        functools.partial(density_kernel, cells),
        out_shape=jax.ShapeDtypeStruct((rows, LANES), jnp.float32),
        in_specs=[smem, vmem],
        out_specs=vmem,
        scratch_shapes=[
            pltpu.VMEM((9, 4, cells, slots), jnp.float32),
            pltpu.VMEM((4 * wide // LANES, len(RODS) * cells, LANES), jnp.float32),
            pltpu.VMEM((wide // LANES, len(RODS) * cells, LANES), jnp.int32),
            pltpu.VMEM((len(RODS) * cells, LANES), jnp.int32),
            pltpu.VMEM((cells, slots), jnp.int32),
            pltpu.VMEM((6 * GROUPS, SUB, LANES), jnp.float32),
            pltpu.VMEM((GROUPS, SUB, LANES), jnp.float32),
            pltpu.VMEM((cells, SUB, slots), jnp.float32),
            pltpu.VMEM((list_tiles + 1, LANES), jnp.int32),
            pltpu.SMEM((list_tiles + 1, LANES), jnp.int32),
            pltpu.SemaphoreType.DMA,
        ],
        compiler_params=pltpu.CompilerParams(vmem_limit_bytes=12 * 1024 * 1024),
        name="density",
    )(rolls, padded)
    return density.reshape(masses.shape)


def solution(mesh):
    in_specs = (
        P(None, "shear", None, "cross", None),
        P("shear", None, "cross", None),
        P("shear", None, "cross"),
        P(),
    )
    out_specs = P("shear", None, "cross", None)
    return jax.shard_map(shards, mesh=mesh, in_specs=in_specs, out_specs=out_specs, check_vma=False)
```

```python
import functools
import jax
import jax.numpy as jnp
from jax import lax
from jax.experimental import pallas as pl
from jax.experimental.pallas import tpu as pltpu
from jax.sharding import PartitionSpec as P

LANES = 128
SUB = 8
GROUPS = 16
RODS = ((0, 0), (0, 1), (1, 0), (1, 1))


def halo_kernel(data_ref, out_ref, send_sems, recv_sems, local_sem):
    shear, cross = lax.axis_index("shear"), lax.axis_index("cross")
    rows, planes = lax.axis_size("shear"), lax.axis_size("cross")
    mesh_ids = pl.DeviceIdType.MESH
    along_y = [(lax.rem(shear + rows - step, rows), cross) for step in (-1, 1)]
    along_z = [(shear, lax.rem(cross + planes - step, planes)) for step in (-1, 1)]
    barrier = pltpu.get_barrier_semaphore()
    for device in along_y + along_z:
        pl.semaphore_signal(barrier, inc=1, device_id=device, device_id_type=mesh_ids)
    own = pltpu.make_async_copy(data_ref, out_ref.at[1, 1], local_sem)
    own.start()
    pl.semaphore_wait(barrier, 4)

    def sent(source, y, z, device):
        slot = 3 * y + z
        copy = pltpu.make_async_remote_copy(
            src_ref=source,
            dst_ref=out_ref.at[y, z],
            send_sem=send_sems.at[slot],
            recv_sem=recv_sems.at[slot],
            device_id=device,
            device_id_type=mesh_ids,
        )
        copy.start()
        return copy

    rows_sent = [sent(data_ref, y, 1, along_y[k]) for k, y in enumerate((0, 2))]
    planes_sent = [sent(data_ref, 1, z, along_z[k]) for k, z in enumerate((0, 2))]
    for k, y in enumerate((0, 2)):
        rows_sent[k].wait_recv()
        for j, z in enumerate((0, 2)):
            planes_sent.append(sent(out_ref.at[y, 1], y, z, along_z[j]))
    for copy in rows_sent:
        copy.wait_send()
    for copy in planes_sent:
        copy.wait()
    own.wait()


def halo(data):
    vmem = pl.BlockSpec(memory_space=pltpu.VMEM)
    return pl.pallas_call(
        halo_kernel,
        out_shape=jax.ShapeDtypeStruct((3, 3) + data.shape, data.dtype),
        in_specs=[vmem],
        out_specs=vmem,
        scratch_shapes=[
            pltpu.SemaphoreType.DMA((9,)),
            pltpu.SemaphoreType.DMA((9,)),
            pltpu.SemaphoreType.DMA,
        ],
        compiler_params=pltpu.CompilerParams(
            collective_id=0, has_side_effects=True, vmem_limit_bytes=4 * 1024 * 1024
        ),
        name="halo",
    )(data)


def density_kernel(
    cells, roll_ref, data_ref, out_ref,
    rel_ref, source_ref, move_ref, total_ref, place_ref, target_ref, acc_ref, sums_ref, list_ref, list_sm, list_sem,
):
    f32, i32 = jnp.float32, jnp.int32
    tiles = data_ref.shape[3] // cells
    slots = tiles * LANES
    wide = 4 * tiles
    list_tiles = list_ref.shape[0] - 1
    near = wide // 2
    half = 0.5

    masks = {}
    for sy in (-1, 0, 1):
        for sz in (-1, 0, 1):
            relation = 3 * (sy + 1) + sz + 1
            parts = []
            for k in range(4):
                value = jnp.concatenate(
                    [data_ref[sy + 1, sz + 1, k, pl.ds(t, cells, stride=tiles), :] for t in range(tiles)], axis=1
                )
                if sy != 0:
                    value = pltpu.roll(value, roll_ref[(sy + 1) // 2], 0)
                parts.append(value)
            y, x, z, mass = parts
            keep = mass > 0.0
            if sy == -1:
                keep = keep & (y >= half)
            elif sy == 1:
                keep = keep & (y <= half)
            if sz == -1:
                keep = keep & (z >= half)
            elif sz == 1:
                keep = keep & (z <= half)
            masks[sy, sz] = keep
            rel_ref[relation, 0] = 4.0 * (y + (sy - half))
            rel_ref[relation, 1] = 4.0 * (x - half)
            rel_ref[relation, 2] = 4.0 * (z + (sz - half))
            rel_ref[relation, 3] = mass
            if sy == 0 and sz == 0:
                own_y, own_x, own_z, own_valid = y, x, z, keep

    octants = []
    for ry, rz in RODS:
        inside = own_valid & ((own_y >= half) if ry else (own_y < half))
        inside = inside & ((own_z >= half) if rz else (own_z < half))
        octants.append(inside & (own_x < half))
        octants.append(inside & (own_x >= half))

    relations = [(sy, sz) for sy in (-1, 0, 1) for sz in (-1, 0, 1)]
    stacked = jnp.concatenate(
        [jnp.where(masks[r], 1.0, 0.0) for r in relations] + [jnp.where(m, 1.0, 0.0) for m in octants], axis=0
    ).astype(jnp.bfloat16)
    row = lax.broadcasted_iota(i32, (slots, slots + LANES), 0)
    col = lax.broadcasted_iota(i32, (slots, slots + LANES), 1)
    triangle = jnp.where((row <= col) | (col >= slots), 1.0, 0.0).astype(jnp.bfloat16)
    ranks = jnp.dot(stacked, triangle, preferred_element_type=f32).astype(i32)

    first = len(relations) * cells
    totals = ranks[first:, slots:]
    groups = (totals + (SUB - 1)) >> 3
    n_oct = len(octants) * cells
    lower = jnp.where(
        lax.broadcasted_iota(i32, (n_oct, n_oct), 1) < lax.broadcasted_iota(i32, (n_oct, n_oct), 0), 1.0, 0.0
    ).astype(jnp.bfloat16)
    base = jnp.dot(lower, groups.astype(f32).astype(jnp.bfloat16), preferred_element_type=f32).astype(i32)
    end = base + groups
    place = jnp.full((cells, slots), -1, i32)
    for o, inside in enumerate(octants):
        begin = base[o * cells:(o + 1) * cells]
        begin = jnp.concatenate([begin] * tiles, axis=1)
        rank = ranks[first + o * cells:first + (o + 1) * cells, :slots]
        place = jnp.where(inside, SUB * begin + rank - 1, place)
    place_ref[...] = place
    cell_row = lax.broadcasted_iota(i32, (cells, LANES), 0)
    rods, words = [], []
    for r, (ry, rz) in enumerate(RODS):
        segments = [(0, 0), (2 * ry - 1, 0), (0, 2 * rz - 1), (2 * ry - 1, 2 * rz - 1)]
        starts, start = [], jnp.zeros((cells, LANES), i32)
        for sy, sz in segments:
            at = (3 * (sy + 1) + sz + 1) * cells
            starts.append(start)
            start = start + ranks[at:at + cells, slots:]
        rods.append((segments, starts, start))
        for side in range(2):
            other = pltpu.roll(cell_row, cells - 1 if side else 1, 0)
            far = jnp.maximum(start, pltpu.roll(start, cells - 1 if side else 1, 0)) > near * LANES
            word = (r * cells + cell_row) + ((r * cells + other) << 7) + (cell_row << 14)
            words.append(word + (side << 19) + jnp.where(far, 1 << 20, 0))
    word = jnp.concatenate(words, axis=0)
    change = pltpu.roll(word, n_oct - 1, 0) - word
    change = jnp.where(lax.broadcasted_iota(i32, (n_oct, LANES), 0) < n_oct - 1, change, 0).astype(f32)
    lane = lax.broadcasted_iota(i32, (n_oct, LANES), 1)
    for j in range(list_tiles):
        passed = jnp.where(end <= lane + (j * LANES - GROUPS), change, 0.0)
        list_ref[j:j + 1, :] = word[:1] + jnp.sum(passed, axis=0, keepdims=True).astype(i32)
    list_ref[list_tiles:list_tiles + 1, :] = end[n_oct - 1:n_oct]

    copy = pltpu.make_async_copy(list_ref, list_sm, list_sem)
    lane = lax.broadcasted_iota(i32, (cells, LANES), 1)
    for r, (segments, starts, total) in enumerate(rods):
        held = slice(r * cells, (r + 1) * cells)
        total_ref[held] = total
        for k, (sy, sz) in enumerate(segments):
            at = (3 * (sy + 1) + sz + 1) * cells
            for t in range(tiles):
                lanes = slice(t * LANES, (t + 1) * LANES)
                word = lane << 10
                if k > 0:
                    shift = (k * slots + t * LANES + 1) + lane - starts[k] - ranks[at:at + cells, lanes]
                    word = word + jnp.where(masks[sy, sz][:, lanes], shift, 0)
                move_ref[k * tiles + t, held] = word
    copy.start()

    lane8 = lax.broadcasted_iota(i32, (SUB, LANES), 1)
    blocks = len(RODS) * cells // SUB

    def stage(k, carry):
        step = 1 << k
        inner = lane8 < LANES - step
        for block in range(blocks):
            held = slice(block * SUB, (block + 1) * SUB)
            words = [move_ref[j, held] for j in range(tiles - 1, wide)]
            turned = [pltpu.roll(w, LANES - step, 1) for w in words] + [jnp.zeros_like(lane8)]
            for j, word in enumerate(words):
                coming = jnp.where(inner, turned[j], turned[j + 1])
                word = jnp.where((word & step) != 0, 0, word)
                move_ref[j + tiles - 1, held] = jnp.where((coming & step) != 0, coming, word)
        return carry

    lax.fori_loop(0, LANES.bit_length() - 1, stage, 0)

    def settle(block, carry):
        rod = block // (cells // SUB)
        top = pl.multiple_of((block - rod * (cells // SUB)) * SUB, SUB)
        held = pl.ds(pl.multiple_of(block * SUB, SUB), SUB)
        ry, rz = 2 * (rod >> 1), 2 * (rod & 1)
        segments = [4, 3 * ry + 1, 3 + rz, 3 * ry + rz]
        words = [move_ref[j, held] for j in range(wide)]
        origin = [w >> 10 for w in words]
        data = []
        for f in range(4):
            raw = [
                rel_ref[segments[j // tiles], f, pl.ds(top, SUB), (j % tiles) * LANES:(j % tiles + 1) * LANES]
                for j in range(wide)
            ]
            moved = []
            for j in range(wide):
                here = raw[j] if j < tiles else jnp.take_along_axis(raw[j], origin[j], axis=1, mode="promise_in_bounds")
                if tiles - 1 <= j < wide - 1:
                    after = jnp.take_along_axis(raw[j + 1], origin[j], axis=1, mode="promise_in_bounds")
                    here = jnp.where(origin[j] >= lane8, here, after)
                moved.append(here)
            data.append(moved)
        step = LANES
        while step < wide * LANES:
            q = step // LANES
            coming = [(w & step) != 0 for w in words[q:]]
            leaving = [(w & step) != 0 for w in words]
            kept = [jnp.where(leaving[j], 0, words[j]) for j in range(wide)]
            words = [jnp.where(coming[j], words[j + q], kept[j]) for j in range(wide - q)] + kept[wide - q:]
            data = [[jnp.where(coming[j], a[j + q], a[j]) for j in range(wide - q)] + a[wide - q:] for a in data]
            step *= 2
        total = total_ref[held]
        for j in range(wide):
            for f in range(3):
                source_ref[f * wide + j, held] = data[f][j]
            source_ref[3 * wide + j, held] = jnp.where(lane8 + j * LANES < total, data[3][j], 0.0)
        return carry

    lax.fori_loop(0, blocks, settle, 0)
    copy.wait()

    sub_row = lax.broadcasted_iota(i32, (SUB, slots), 0)
    own = 4

    def entries(body):
        at = (body + 1) * GROUPS
        line, at = at >> 7, at & (LANES - 1)
        return [list_sm[line, at + k] for k in range(GROUPS)]

    def chosen(word, g):
        cell = (word >> 14) & 31
        place_row = jnp.broadcast_to(place_ref[pl.ds(cell, 1), :], (SUB, slots))
        return cell, place_row == sub_row + g * SUB

    def gather(body):
        buffer = (body & 1) * (3 * GROUPS)
        for k, word in enumerate(entries(body)):
            cell, mask = chosen(word, body * GROUPS + k)
            for f in range(3):
                value = jnp.where(mask, rel_ref[own, f, pl.ds(cell, 1), :], 0.0)
                value = sum(value[:, t * LANES:(t + 1) * LANES] for t in range(tiles))
                target_ref[buffer + 3 * k + f] = jnp.broadcast_to(jnp.sum(value, axis=1, keepdims=True), (SUB, LANES))

    def scatter(body):
        for k, word in enumerate(entries(body)):
            cell, mask = chosen(word, body * GROUPS + k)
            total = jnp.sum(acc_ref[k], axis=1, keepdims=True)
            sums_ref[cell] = sums_ref[cell] + jnp.where(mask, total, 0.0)

    def part(line, at, ty, tx, tz, acc):
        y, x, z, mass = (source_ref[f * wide + at, pl.ds(line, SUB, stride=0)] for f in range(4))
        dy, dx, dz = y - ty, x - tx, z - tz
        squared = dy * dy + dx * dx + dz * dz
        q = pl.reciprocal(lax.rsqrt(squared))
        outer = jnp.maximum(2.0 - q, 0.0)
        value = jnp.minimum(4.0 - 3.0 * (squared * outer), outer * outer * outer)
        return acc + mass * value

    def compute(body, k, word, begin, finish, acc):
        at_target = (body & 1) * (3 * GROUPS) + 3 * k
        line, other = word & 127, (word >> 7) & 127
        offset = jnp.where((word & (1 << 19)) != 0, -4.0, 4.0)
        ty, tx, tz = (target_ref[at_target + f] for f in range(3))
        moved = tx + offset
        for at in range(begin, finish):
            acc = part(line, at, ty, tx, tz, acc)
            acc = part(other, at, ty, moved, tz, acc)
        acc_ref[k] = acc

    sums_ref[...] = jnp.zeros(sums_ref.shape, f32)
    acc_ref[...] = jnp.zeros(acc_ref.shape, f32)
    bodies = (list_sm[list_tiles, 0] + (GROUPS - 1)) // GROUPS
    gather(0)

    def body_step(body, carry):
        words = entries(body)
        scatter(body - 1)
        for k, word in enumerate(words):
            compute(body, k, word, 0, near, jnp.zeros((SUB, LANES), f32))
        gather(body + 1)
        flags = words[0]
        for word in words[1:]:
            flags = flags | word

        @pl.when((flags & (1 << 20)) != 0)
        def _():
            def far_step(k, carry):
                at = (body + 1) * GROUPS
                word = list_sm[at >> 7, (at & (LANES - 1)) + k]

                @pl.when((word & (1 << 20)) != 0)
                def _():
                    compute(body, k, word, near, wide, acc_ref[k])

                return carry

            lax.fori_loop(0, GROUPS, far_step, 0)

        return carry

    lax.fori_loop(0, bodies, body_step, 0)
    scatter(bodies - 1)
    for cell in range(cells):
        total = jnp.sum(sums_ref[cell], axis=0, keepdims=True) * (16.0 / 3.141592653589793)
        for t in range(tiles):
            out_ref[cell * tiles + t:cell * tiles + t + 1, :] = total[:, t * LANES:(t + 1) * LANES]


def shards(positions, masses, counts, shear_offset):
    cells_y, cells, cells_z, slots = masses.shape
    assert cells_y == 1 and cells_z == 1 and slots % LANES == 0
    tiles = slots // LANES
    rows = cells * tiles
    slot = lax.broadcasted_iota(jnp.int32, (rows, LANES), 1)
    slot = slot + LANES * lax.rem(lax.broadcasted_iota(jnp.int32, (rows, LANES), 0), tiles)
    held = jnp.repeat(counts.reshape(cells), tiles)[:, None]
    weight = jnp.where(slot < held, masses.reshape(rows, LANES), jnp.float32(0.0))
    data = jnp.concatenate([positions.reshape(3, rows, LANES), weight[None]], 0)
    padded = halo(data)
    offset = shear_offset[0]
    shear_index = lax.axis_index("shear")
    cycle = lax.axis_size("shear")
    low = jnp.where(shear_index == 0, offset, 0) % cells
    high = jnp.where(shear_index == cycle - 1, -offset, 0) % cells
    rolls = jnp.stack([low, high]).astype(jnp.int32)

    octants = 2 * len(RODS)
    most_groups = cells * (slots // SUB + octants - 1)
    list_tiles = -(-(most_groups + 3 * GROUPS) // LANES)
    wide = 4 * slots
    smem = pl.BlockSpec(memory_space=pltpu.SMEM)
    vmem = pl.BlockSpec(memory_space=pltpu.VMEM)
    density = pl.pallas_call(
        functools.partial(density_kernel, cells),
        out_shape=jax.ShapeDtypeStruct((rows, LANES), jnp.float32),
        in_specs=[smem, vmem],
        out_specs=vmem,
        scratch_shapes=[
            pltpu.VMEM((9, 4, cells, slots), jnp.float32),
            pltpu.VMEM((4 * wide // LANES, len(RODS) * cells, LANES), jnp.float32),
            pltpu.VMEM((wide // LANES, len(RODS) * cells, LANES), jnp.int32),
            pltpu.VMEM((len(RODS) * cells, LANES), jnp.int32),
            pltpu.VMEM((cells, slots), jnp.int32),
            pltpu.VMEM((6 * GROUPS, SUB, LANES), jnp.float32),
            pltpu.VMEM((GROUPS, SUB, LANES), jnp.float32),
            pltpu.VMEM((cells, SUB, slots), jnp.float32),
            pltpu.VMEM((list_tiles + 1, LANES), jnp.int32),
            pltpu.SMEM((list_tiles + 1, LANES), jnp.int32),
            pltpu.SemaphoreType.DMA,
        ],
        compiler_params=pltpu.CompilerParams(vmem_limit_bytes=12 * 1024 * 1024),
        name="density",
    )(rolls, padded)
    return density.reshape(masses.shape)


def solution(mesh):
    in_specs = (
        P(None, "shear", None, "cross", None),
        P("shear", None, "cross", None),
        P("shear", None, "cross"),
        P(),
    )
    out_specs = P("shear", None, "cross", None)
    return jax.shard_map(shards, mesh=mesh, in_specs=in_specs, out_specs=out_specs, check_vma=False)
```

```python
import functools
import jax
import jax.numpy as jnp
from jax import lax
from jax.experimental import pallas as pl
from jax.experimental.pallas import tpu as pltpu
from jax.sharding import PartitionSpec as P

LANES = 128
SUB = 8
GROUPS = 16
RODS = ((0, 0), (0, 1), (1, 0), (1, 1))


def halo_kernel(data_ref, out_ref, send_sems, recv_sems, local_sem):
    shear, cross = lax.axis_index("shear"), lax.axis_index("cross")
    rows, planes = lax.axis_size("shear"), lax.axis_size("cross")
    mesh_ids = pl.DeviceIdType.MESH
    along_y = [(lax.rem(shear + rows - step, rows), cross) for step in (-1, 1)]
    along_z = [(shear, lax.rem(cross + planes - step, planes)) for step in (-1, 1)]
    barrier = pltpu.get_barrier_semaphore()
    for device in along_y + along_z:
        pl.semaphore_signal(barrier, inc=1, device_id=device, device_id_type=mesh_ids)
    own = pltpu.make_async_copy(data_ref, out_ref.at[1, 1], local_sem)
    own.start()
    pl.semaphore_wait(barrier, 4)

    def sent(source, y, z, device):
        slot = 3 * y + z
        copy = pltpu.make_async_remote_copy(
            src_ref=source,
            dst_ref=out_ref.at[y, z],
            send_sem=send_sems.at[slot],
            recv_sem=recv_sems.at[slot],
            device_id=device,
            device_id_type=mesh_ids,
        )
        copy.start()
        return copy

    rows_sent = [sent(data_ref, y, 1, along_y[k]) for k, y in enumerate((0, 2))]
    planes_sent = [sent(data_ref, 1, z, along_z[k]) for k, z in enumerate((0, 2))]
    for k, y in enumerate((0, 2)):
        rows_sent[k].wait_recv()
        for j, z in enumerate((0, 2)):
            planes_sent.append(sent(out_ref.at[y, 1], y, z, along_z[j]))
    for copy in rows_sent:
        copy.wait_send()
    for copy in planes_sent:
        copy.wait()
    own.wait()


def halo(data):
    vmem = pl.BlockSpec(memory_space=pltpu.VMEM)
    return pl.pallas_call(
        halo_kernel,
        out_shape=jax.ShapeDtypeStruct((3, 3) + data.shape, data.dtype),
        in_specs=[vmem],
        out_specs=vmem,
        scratch_shapes=[
            pltpu.SemaphoreType.DMA((9,)),
            pltpu.SemaphoreType.DMA((9,)),
            pltpu.SemaphoreType.DMA,
        ],
        compiler_params=pltpu.CompilerParams(
            collective_id=0, has_side_effects=True, vmem_limit_bytes=4 * 1024 * 1024
        ),
        name="halo",
    )(data)


def density_kernel(
    cells, roll_ref, data_ref, out_ref,
    rel_ref, source_ref, move_ref, total_ref, place_ref, own_ref, target_ref, acc_ref, list_ref, list_sm, list_sem, *sums_refs,
):
    f32, i32 = jnp.float32, jnp.int32
    tiles = data_ref.shape[3] // cells
    slots = tiles * LANES
    wide = 4 * tiles
    list_tiles = list_ref.shape[0] - 1
    near = wide // 2
    small = near - 1
    half = 0.5

    masks = {}
    for sy in (-1, 0, 1):
        for sz in (-1, 0, 1):
            relation = 3 * (sy + 1) + sz + 1
            parts = []
            for k in range(4):
                value = jnp.concatenate(
                    [data_ref[sy + 1, sz + 1, k, pl.ds(t, cells, stride=tiles), :] for t in range(tiles)], axis=1
                )
                if sy != 0:
                    value = pltpu.roll(value, roll_ref[(sy + 1) // 2], 0)
                parts.append(value)
            y, x, z, mass = parts
            keep = mass > 0.0
            if sy == -1:
                keep = keep & (y >= half)
            elif sy == 1:
                keep = keep & (y <= half)
            if sz == -1:
                keep = keep & (z >= half)
            elif sz == 1:
                keep = keep & (z <= half)
            masks[sy, sz] = keep
            rel_ref[relation, 0] = 4.0 * (y + (sy - half))
            rel_ref[relation, 1] = 4.0 * (x - half)
            rel_ref[relation, 2] = 4.0 * (z + (sz - half))
            rel_ref[relation, 3] = mass
            if sy == 0 and sz == 0:
                own_y, own_x, own_z, own_valid = y, x, z, keep

    octants = []
    for ry, rz in RODS:
        inside = own_valid & ((own_y >= half) if ry else (own_y < half))
        inside = inside & ((own_z >= half) if rz else (own_z < half))
        octants.append(inside & (own_x < half))
        octants.append(inside & (own_x >= half))

    relations = [(sy, sz) for sy in (-1, 0, 1) for sz in (-1, 0, 1)]
    stacked = jnp.concatenate(
        [jnp.where(masks[r], 1.0, 0.0) for r in relations] + [jnp.where(m, 1.0, 0.0) for m in octants], axis=0
    ).astype(jnp.bfloat16)
    row = lax.broadcasted_iota(i32, (slots, slots + LANES), 0)
    col = lax.broadcasted_iota(i32, (slots, slots + LANES), 1)
    triangle = jnp.where((row <= col) | (col >= slots), 1.0, 0.0).astype(jnp.bfloat16)
    ranks = jnp.dot(stacked, triangle, preferred_element_type=f32).astype(i32)

    first = len(relations) * cells
    n_oct = len(octants) * cells
    cell_row = lax.broadcasted_iota(i32, (cells, LANES), 0)
    rods, words, ranking = [], [], []
    for r, (ry, rz) in enumerate(RODS):
        segments = [(0, 0), (2 * ry - 1, 0), (0, 2 * rz - 1), (2 * ry - 1, 2 * rz - 1)]
        starts, start = [], jnp.zeros((cells, LANES), i32)
        for sy, sz in segments:
            at = (3 * (sy + 1) + sz + 1) * cells
            starts.append(start)
            start = start + ranks[at:at + cells, slots:]
        rods.append((segments, starts, start))
        for side in range(2):
            turn = cells - 1 if side else 1
            other = pltpu.roll(cell_row, turn, 0)
            most = jnp.maximum(start, pltpu.roll(start, turn, 0))
            word = (r * cells + cell_row) + ((r * cells + other) << 7) + (cell_row << 14)
            words.append(word + (side << 19) + jnp.where(most > near * LANES, 1 << 20, 0))
            ranking.append(jnp.where(most > small * LANES, n_oct, 0))
    word = jnp.concatenate(words, axis=0).astype(f32)

    totals = ranks[first:, slots:]
    groups = ((totals + (SUB - 1)) >> 3).astype(f32)
    oct_row = lax.broadcasted_iota(i32, (n_oct, LANES), 0)
    oct_lane = lax.broadcasted_iota(i32, (n_oct, LANES), 1)
    light = jnp.concatenate(ranking, axis=0)
    order = (light + oct_row).astype(f32)
    order_lane = jnp.sum(jnp.where(oct_row == oct_lane, order, 0.0), axis=0, keepdims=True)
    lower = jnp.where(order_lane < order, 1.0, 0.0).astype(jnp.bfloat16)
    base = jnp.dot(lower, groups.astype(jnp.bfloat16), preferred_element_type=f32)
    end = base + groups
    place = jnp.full((cells, slots), -1, i32)
    for o, inside in enumerate(octants):
        begin = base[o * cells:(o + 1) * cells].astype(i32)
        begin = jnp.concatenate([begin] * tiles, axis=1)
        rank = ranks[first + o * cells:first + (o + 1) * cells, :slots]
        place = jnp.where(inside, SUB * begin + rank - 1, place)
    for j in range(list_tiles):
        at = (oct_lane + (j * LANES - GROUPS)).astype(f32)
        held = jnp.sum(jnp.where((base <= at) & (at < end), word, 0.0), axis=0, keepdims=True)
        list_ref[j:j + 1, :] = held.astype(i32)
    every = jnp.sum(groups, axis=0, keepdims=True)
    few = jnp.sum(jnp.where(light == 0, groups, 0.0), axis=0, keepdims=True)
    list_ref[list_tiles:list_tiles + 1, :] = jnp.where(oct_lane[:1] == 0, every, few).astype(i32)

    for t in range(tiles):
        lanes = slice(t * LANES, (t + 1) * LANES)
        place_ref[t] = place[:, lanes]
        for f in range(3):
            own_ref[f * tiles + t] = rel_ref[4, f, :, lanes]
    copies = [
        pltpu.make_async_copy(list_ref.at[j], list_sm.at[pl.ds(j * LANES, LANES)], list_sem.at[j])
        for j in range(list_tiles + 1)
    ]
    lane = lax.broadcasted_iota(i32, (cells, LANES), 1)
    for r, (segments, starts, total) in enumerate(rods):
        held = slice(r * cells, (r + 1) * cells)
        total_ref[held] = total
        for k, (sy, sz) in enumerate(segments):
            at = (3 * (sy + 1) + sz + 1) * cells
            for t in range(tiles):
                lanes = slice(t * LANES, (t + 1) * LANES)
                word = lane << 10
                if k > 0:
                    shift = (k * slots + t * LANES + 1) + lane - starts[k] - ranks[at:at + cells, lanes]
                    word = word + jnp.where(masks[sy, sz][:, lanes], shift, 0)
                move_ref[k * tiles + t, held] = word
    for copy in copies:
        copy.start()

    lane8 = lax.broadcasted_iota(i32, (SUB, LANES), 1)
    blocks = len(RODS) * cells // SUB

    def stage(k, carry):
        step = 1 << k
        inner = lane8 < LANES - step
        for block in range(blocks):
            held = slice(block * SUB, (block + 1) * SUB)
            words = [move_ref[j, held] for j in range(tiles - 1, wide)]
            turned = [pltpu.roll(w, LANES - step, 1) for w in words] + [jnp.zeros_like(lane8)]
            for j, word in enumerate(words):
                coming = jnp.where(inner, turned[j], turned[j + 1])
                word = jnp.where((word & step) != 0, 0, word)
                move_ref[j + tiles - 1, held] = jnp.where((coming & step) != 0, coming, word)
        return carry

    lax.fori_loop(0, LANES.bit_length() - 1, stage, 0)

    def settle(block, carry):
        rod = block // (cells // SUB)
        top = pl.multiple_of((block - rod * (cells // SUB)) * SUB, SUB)
        held = pl.ds(pl.multiple_of(block * SUB, SUB), SUB)
        ry, rz = 2 * (rod >> 1), 2 * (rod & 1)
        segments = [4, 3 * ry + 1, 3 + rz, 3 * ry + rz]
        words = [move_ref[j, held] for j in range(wide)]
        origin = [w >> 10 for w in words]
        data = []
        for f in range(4):
            raw = [
                rel_ref[segments[j // tiles], f, pl.ds(top, SUB), (j % tiles) * LANES:(j % tiles + 1) * LANES]
                for j in range(wide)
            ]
            moved = []
            for j in range(wide):
                here = raw[j] if j < tiles else jnp.take_along_axis(raw[j], origin[j], axis=1, mode="promise_in_bounds")
                if tiles - 1 <= j < wide - 1:
                    after = jnp.take_along_axis(raw[j + 1], origin[j], axis=1, mode="promise_in_bounds")
                    here = jnp.where(origin[j] >= lane8, here, after)
                moved.append(here)
            data.append(moved)
        step = LANES
        while step < wide * LANES:
            q = step // LANES
            coming = [(w & step) != 0 for w in words[q:]]
            leaving = [(w & step) != 0 for w in words]
            kept = [jnp.where(leaving[j], 0, words[j]) for j in range(wide)]
            words = [jnp.where(coming[j], words[j + q], kept[j]) for j in range(wide - q)] + kept[wide - q:]
            data = [[jnp.where(coming[j], a[j + q], a[j]) for j in range(wide - q)] + a[wide - q:] for a in data]
            step *= 2
        total = total_ref[held]
        for j in range(wide):
            for f in range(3):
                source_ref[f * wide + j, held] = data[f][j]
            source_ref[3 * wide + j, held] = jnp.where(lane8 + j * LANES < total, data[3][j], 0.0)
        return carry

    lax.fori_loop(0, blocks, settle, 0)
    for copy in copies:
        copy.wait()

    sub_row = lax.broadcasted_iota(i32, (SUB, LANES), 0)

    def entries(body):
        return [list_sm[(body + 1) * GROUPS + k] for k in range(GROUPS)]

    def chosen(word, g):
        cell = (word >> 14) & 31
        rows = sub_row + g * SUB
        return cell, [place_ref[t, pl.ds(cell, SUB, stride=0)] == rows for t in range(tiles)]

    def gather(body):
        buffer = (body & 1) * (3 * GROUPS)
        for k, word in enumerate(entries(body)):
            cell, mask = chosen(word, body * GROUPS + k)
            for f in range(3):
                value = sum(
                    jnp.where(mask[t], own_ref[f * tiles + t, pl.ds(cell, SUB, stride=0)], 0.0) for t in range(tiles)
                )
                target_ref[buffer + 3 * k + f] = jnp.broadcast_to(jnp.sum(value, axis=1, keepdims=True), (SUB, LANES))

    def scatter(body):
        for k, word in enumerate(entries(body)):
            cell, mask = chosen(word, body * GROUPS + k)
            total = jnp.sum(acc_ref[k], axis=1, keepdims=True)
            for t in range(tiles):
                at = cell * tiles + t
                held = sums_refs[k % len(sums_refs)]
                held[at] = held[at] + jnp.where(mask[t], total, 0.0)

    def part(line, at, ty, tx, tz, acc):
        y, x, z, mass = (source_ref[f * wide + at, pl.ds(line, SUB, stride=0)] for f in range(4))
        dy, dx, dz = y - ty, x - tx, z - tz
        squared = dy * dy + dx * dx + dz * dz
        q = pl.reciprocal(lax.rsqrt(squared))
        outer = jnp.maximum(2.0 - q, 0.0)
        value = jnp.minimum(4.0 - 3.0 * (squared * outer), outer * outer * outer)
        return acc + mass * value

    def compute(body, k, word, begin, finish, acc):
        at_target = (body & 1) * (3 * GROUPS) + 3 * k
        line, other = word & 127, (word >> 7) & 127
        offset = jnp.where((word & (1 << 19)) != 0, -4.0, 4.0)
        ty, tx, tz = (target_ref[at_target + f] for f in range(3))
        moved = tx + offset
        for at in range(begin, finish):
            acc = part(line, at, ty, tx, tz, acc)
            acc = part(other, at, ty, moved, tz, acc)
        acc_ref[k] = acc

    for held in sums_refs:
        held[...] = jnp.zeros(held.shape, f32)
    acc_ref[...] = jnp.zeros(acc_ref.shape, f32)
    bodies = (list_sm[list_tiles * LANES] + (GROUPS - 1)) // GROUPS
    light_bodies = list_sm[list_tiles * LANES + 1] // GROUPS
    gather(0)

    def body_step(limit, body, carry):
        words = entries(body)
        scatter(body - 1)
        for k, word in enumerate(words):
            compute(body, k, word, 0, limit, jnp.zeros((SUB, LANES), f32))
        gather(body + 1)
        if limit == small:
            return carry
        flags = words[0]
        for word in words[1:]:
            flags = flags | word

        @pl.when((flags & (1 << 20)) != 0)
        def _():
            def far_step(k, carry):
                word = list_sm[(body + 1) * GROUPS + k]

                @pl.when((word & (1 << 20)) != 0)
                def _():
                    compute(body, k, word, near, wide, acc_ref[k])

                return carry

            lax.fori_loop(0, GROUPS, far_step, 0)

        return carry

    lax.fori_loop(0, light_bodies, functools.partial(body_step, small), 0)
    lax.fori_loop(light_bodies, bodies, functools.partial(body_step, near), 0)
    scatter(bodies - 1)
    for at in range(cells * tiles):
        out_ref[at:at + 1, :] = jnp.sum(sum(held[at] for held in sums_refs), axis=0, keepdims=True) * (16.0 / 3.141592653589793)


def shards(positions, masses, counts, shear_offset):
    cells_y, cells, cells_z, slots = masses.shape
    assert cells_y == 1 and cells_z == 1 and slots % LANES == 0
    tiles = slots // LANES
    rows = cells * tiles
    slot = lax.broadcasted_iota(jnp.int32, (rows, LANES), 1)
    slot = slot + LANES * lax.rem(lax.broadcasted_iota(jnp.int32, (rows, LANES), 0), tiles)
    held = jnp.repeat(counts.reshape(cells), tiles)[:, None]
    weight = jnp.where(slot < held, masses.reshape(rows, LANES), jnp.float32(0.0))
    data = jnp.concatenate([positions.reshape(3, rows, LANES), weight[None]], 0)
    padded = halo(data)
    offset = shear_offset[0]
    shear_index = lax.axis_index("shear")
    cycle = lax.axis_size("shear")
    low = jnp.where(shear_index == 0, offset, 0) % cells
    high = jnp.where(shear_index == cycle - 1, -offset, 0) % cells
    rolls = jnp.stack([low, high]).astype(jnp.int32)

    octants = 2 * len(RODS)
    most_groups = cells * (slots // SUB + octants - 1)
    list_tiles = -(-(most_groups + 3 * GROUPS) // LANES)
    wide = 4 * slots
    smem = pl.BlockSpec(memory_space=pltpu.SMEM)
    vmem = pl.BlockSpec(memory_space=pltpu.VMEM)
    density = pl.pallas_call(
        functools.partial(density_kernel, cells),
        out_shape=jax.ShapeDtypeStruct((rows, LANES), jnp.float32),
        in_specs=[smem, vmem],
        out_specs=vmem,
        scratch_shapes=[
            pltpu.VMEM((9, 4, cells, slots), jnp.float32),
            pltpu.VMEM((4 * wide // LANES, len(RODS) * cells, LANES), jnp.float32),
            pltpu.VMEM((wide // LANES, len(RODS) * cells, LANES), jnp.int32),
            pltpu.VMEM((len(RODS) * cells, LANES), jnp.int32),
            pltpu.VMEM((tiles, cells, LANES), jnp.int32),
            pltpu.VMEM((3 * tiles, cells, LANES), jnp.float32),
            pltpu.VMEM((6 * GROUPS, SUB, LANES), jnp.float32),
            pltpu.VMEM((GROUPS, SUB, LANES), jnp.float32),
            pltpu.VMEM((list_tiles + 1, LANES), jnp.int32),
            pltpu.SMEM(((list_tiles + 1) * LANES,), jnp.int32),
            pltpu.SemaphoreType.DMA((list_tiles + 1,)),
        ] + 4 * [pltpu.VMEM((rows, SUB, LANES), jnp.float32)],
        compiler_params=pltpu.CompilerParams(vmem_limit_bytes=12 * 1024 * 1024),
        name="density",
    )(rolls, padded)
    return density.reshape(masses.shape)


def solution(mesh):
    in_specs = (
        P(None, "shear", None, "cross", None),
        P("shear", None, "cross", None),
        P("shear", None, "cross"),
        P(),
    )
    out_specs = P("shear", None, "cross", None)
    return jax.shard_map(shards, mesh=mesh, in_specs=in_specs, out_specs=out_specs, check_vma=False)
```

```python
import functools
import jax
import jax.numpy as jnp
from jax import lax
from jax.experimental import pallas as pl
from jax.experimental.pallas import tpu as pltpu
from jax.sharding import PartitionSpec as P

LANES = 128
SUB = 8
GROUPS = 16
RODS = ((0, 0), (0, 1), (1, 0), (1, 1))


def halo_kernel(data_ref, out_ref, send_sems, recv_sems, local_sem):
    shear, cross = lax.axis_index("shear"), lax.axis_index("cross")
    rows, planes = lax.axis_size("shear"), lax.axis_size("cross")
    mesh_ids = pl.DeviceIdType.MESH
    along_y = [(lax.rem(shear + rows - step, rows), cross) for step in (-1, 1)]
    along_z = [(shear, lax.rem(cross + planes - step, planes)) for step in (-1, 1)]
    barrier = pltpu.get_barrier_semaphore()
    for device in along_y + along_z:
        pl.semaphore_signal(barrier, inc=1, device_id=device, device_id_type=mesh_ids)
    own = pltpu.make_async_copy(data_ref, out_ref.at[1, 1], local_sem)
    own.start()
    pl.semaphore_wait(barrier, 4)

    def sent(source, y, z, device):
        slot = 3 * y + z
        copy = pltpu.make_async_remote_copy(
            src_ref=source,
            dst_ref=out_ref.at[y, z],
            send_sem=send_sems.at[slot],
            recv_sem=recv_sems.at[slot],
            device_id=device,
            device_id_type=mesh_ids,
        )
        copy.start()
        return copy

    rows_sent = [sent(data_ref, y, 1, along_y[k]) for k, y in enumerate((0, 2))]
    planes_sent = [sent(data_ref, 1, z, along_z[k]) for k, z in enumerate((0, 2))]
    for k, y in enumerate((0, 2)):
        rows_sent[k].wait_recv()
        for j, z in enumerate((0, 2)):
            planes_sent.append(sent(out_ref.at[y, 1], y, z, along_z[j]))
    for copy in rows_sent:
        copy.wait_send()
    for copy in planes_sent:
        copy.wait()
    own.wait()


def halo(data):
    vmem = pl.BlockSpec(memory_space=pltpu.VMEM)
    return pl.pallas_call(
        halo_kernel,
        out_shape=jax.ShapeDtypeStruct((3, 3) + data.shape, data.dtype),
        in_specs=[vmem],
        out_specs=vmem,
        scratch_shapes=[
            pltpu.SemaphoreType.DMA((9,)),
            pltpu.SemaphoreType.DMA((9,)),
            pltpu.SemaphoreType.DMA,
        ],
        compiler_params=pltpu.CompilerParams(
            collective_id=0, has_side_effects=True, vmem_limit_bytes=4 * 1024 * 1024
        ),
        name="halo",
    )(data)


def density_kernel(
    cells, roll_ref, data_ref, out_ref,
    rel_ref, source_ref, move_ref, total_ref, place_ref, own_ref, target_ref, front_ref, back_ref, acc_ref, list_ref, list_sm, list_sem, *sums_refs,
):
    f32, i32 = jnp.float32, jnp.int32
    tiles = data_ref.shape[3] // cells
    slots = tiles * LANES
    wide = 4 * tiles
    list_tiles = list_ref.shape[0] - 1
    near = wide // 2
    small = near - 1
    half_groups = GROUPS // 2
    half = 0.5

    masks = {}
    for sy in (-1, 0, 1):
        for sz in (-1, 0, 1):
            relation = 3 * (sy + 1) + sz + 1
            parts = []
            for k in range(4):
                value = jnp.concatenate(
                    [data_ref[sy + 1, sz + 1, k, pl.ds(t, cells, stride=tiles), :] for t in range(tiles)], axis=1
                )
                if sy != 0:
                    value = pltpu.roll(value, roll_ref[(sy + 1) // 2], 0)
                parts.append(value)
            y, x, z, mass = parts
            keep = mass > 0.0
            if sy == -1:
                keep = keep & (y >= half)
            elif sy == 1:
                keep = keep & (y <= half)
            if sz == -1:
                keep = keep & (z >= half)
            elif sz == 1:
                keep = keep & (z <= half)
            masks[sy, sz] = keep
            rel_ref[relation, 0] = 4.0 * (y + (sy - half))
            rel_ref[relation, 1] = 4.0 * (x - half)
            rel_ref[relation, 2] = 4.0 * (z + (sz - half))
            rel_ref[relation, 3] = mass
            if sy == 0 and sz == 0:
                own_y, own_x, own_z, own_valid = y, x, z, keep

    octants = []
    for ry, rz in RODS:
        inside = own_valid & ((own_y >= half) if ry else (own_y < half))
        inside = inside & ((own_z >= half) if rz else (own_z < half))
        octants.append(inside & (own_x < half))
        octants.append(inside & (own_x >= half))

    relations = [(sy, sz) for sy in (-1, 0, 1) for sz in (-1, 0, 1)]
    stacked = jnp.concatenate(
        [jnp.where(masks[r], 1.0, 0.0) for r in relations] + [jnp.where(m, 1.0, 0.0) for m in octants], axis=0
    ).astype(jnp.bfloat16)
    row = lax.broadcasted_iota(i32, (slots, slots + LANES), 0)
    col = lax.broadcasted_iota(i32, (slots, slots + LANES), 1)
    triangle = jnp.where((row <= col) | (col >= slots), 1.0, 0.0).astype(jnp.bfloat16)
    ranks = jnp.dot(stacked, triangle, preferred_element_type=f32).astype(i32)

    first = len(relations) * cells
    n_oct = len(octants) * cells
    cell_row = lax.broadcasted_iota(i32, (cells, LANES), 0)
    rods, words, ranking = [], [], []
    for r, (ry, rz) in enumerate(RODS):
        segments = [(0, 0), (2 * ry - 1, 0), (0, 2 * rz - 1), (2 * ry - 1, 2 * rz - 1)]
        starts, start = [], jnp.zeros((cells, LANES), i32)
        for sy, sz in segments:
            at = (3 * (sy + 1) + sz + 1) * cells
            starts.append(start)
            start = start + ranks[at:at + cells, slots:]
        rods.append((segments, starts, start))
        for side in range(2):
            turn = cells - 1 if side else 1
            other = pltpu.roll(cell_row, turn, 0)
            most = jnp.maximum(start, pltpu.roll(start, turn, 0))
            word = (r * cells + cell_row) + ((r * cells + other) << 7) + (cell_row << 14)
            words.append(word + (side << 19) + jnp.where(most > near * LANES, 1 << 20, 0))
            ranking.append(jnp.where(most > small * LANES, n_oct, 0))
    word = jnp.concatenate(words, axis=0).astype(f32)

    totals = ranks[first:, slots:]
    groups = ((totals + (SUB - 1)) >> 3).astype(f32)
    oct_row = lax.broadcasted_iota(i32, (n_oct, LANES), 0)
    oct_lane = lax.broadcasted_iota(i32, (n_oct, LANES), 1)
    light = jnp.concatenate(ranking, axis=0)
    order = (light + oct_row).astype(f32)
    order_lane = jnp.sum(jnp.where(oct_row == oct_lane, order, 0.0), axis=0, keepdims=True)
    lower = jnp.where(order_lane < order, 1.0, 0.0).astype(jnp.bfloat16)
    base = jnp.dot(lower, groups.astype(jnp.bfloat16), preferred_element_type=f32)
    end = base + groups
    place = jnp.full((cells, slots), -1, i32)
    for o, inside in enumerate(octants):
        begin = base[o * cells:(o + 1) * cells].astype(i32)
        begin = jnp.concatenate([begin] * tiles, axis=1)
        rank = ranks[first + o * cells:first + (o + 1) * cells, :slots]
        place = jnp.where(inside, SUB * begin + rank - 1, place)
    for j in range(list_tiles):
        at = (oct_lane + (j * LANES - GROUPS)).astype(f32)
        held = jnp.sum(jnp.where((base <= at) & (at < end), word, 0.0), axis=0, keepdims=True)
        list_ref[j:j + 1, :] = held.astype(i32)
    every = jnp.sum(groups, axis=0, keepdims=True)
    few = jnp.sum(jnp.where(light == 0, groups, 0.0), axis=0, keepdims=True)
    list_ref[list_tiles:list_tiles + 1, :] = jnp.where(oct_lane[:1] == 0, every, few).astype(i32)

    for t in range(tiles):
        lanes = slice(t * LANES, (t + 1) * LANES)
        place_ref[t] = place[:, lanes]
        for f in range(3):
            own_ref[f * tiles + t] = rel_ref[4, f, :, lanes]
    copies = [
        pltpu.make_async_copy(list_ref.at[j], list_sm.at[pl.ds(j * LANES, LANES)], list_sem.at[j])
        for j in range(list_tiles + 1)
    ]
    lane = lax.broadcasted_iota(i32, (cells, LANES), 1)
    for r, (segments, starts, total) in enumerate(rods):
        held = slice(r * cells, (r + 1) * cells)
        total_ref[held] = total
        for k, (sy, sz) in enumerate(segments):
            at = (3 * (sy + 1) + sz + 1) * cells
            for t in range(tiles):
                lanes = slice(t * LANES, (t + 1) * LANES)
                word = lane << 10
                if k > 0:
                    shift = (k * slots + t * LANES + 1) + lane - starts[k] - ranks[at:at + cells, lanes]
                    word = word + jnp.where(masks[sy, sz][:, lanes], shift, 0)
                move_ref[k * tiles + t, held] = word
    for copy in copies:
        copy.start()

    lane8 = lax.broadcasted_iota(i32, (SUB, LANES), 1)
    blocks = len(RODS) * cells // SUB

    def stage(k, carry):
        step = 1 << k
        inner = lane8 < LANES - step
        for block in range(blocks):
            held = slice(block * SUB, (block + 1) * SUB)
            words = [move_ref[j, held] for j in range(tiles - 1, wide)]
            turned = [pltpu.roll(w, LANES - step, 1) for w in words] + [jnp.zeros_like(lane8)]
            for j, word in enumerate(words):
                coming = jnp.where(inner, turned[j], turned[j + 1])
                word = jnp.where((word & step) != 0, 0, word)
                move_ref[j + tiles - 1, held] = jnp.where((coming & step) != 0, coming, word)
        return carry

    lax.fori_loop(0, LANES.bit_length() - 1, stage, 0)

    def settle(block, carry):
        rod = block // (cells // SUB)
        top = pl.multiple_of((block - rod * (cells // SUB)) * SUB, SUB)
        held = pl.ds(pl.multiple_of(block * SUB, SUB), SUB)
        ry, rz = 2 * (rod >> 1), 2 * (rod & 1)
        segments = [4, 3 * ry + 1, 3 + rz, 3 * ry + rz]
        words = [move_ref[j, held] for j in range(wide)]
        origin = [w >> 10 for w in words]
        data = []
        for f in range(4):
            raw = [
                rel_ref[segments[j // tiles], f, pl.ds(top, SUB), (j % tiles) * LANES:(j % tiles + 1) * LANES]
                for j in range(wide)
            ]
            moved = []
            for j in range(wide):
                here = raw[j] if j < tiles else jnp.take_along_axis(raw[j], origin[j], axis=1, mode="promise_in_bounds")
                if tiles - 1 <= j < wide - 1:
                    after = jnp.take_along_axis(raw[j + 1], origin[j], axis=1, mode="promise_in_bounds")
                    here = jnp.where(origin[j] >= lane8, here, after)
                moved.append(here)
            data.append(moved)
        step = LANES
        while step < wide * LANES:
            q = step // LANES
            coming = [(w & step) != 0 for w in words[q:]]
            leaving = [(w & step) != 0 for w in words]
            kept = [jnp.where(leaving[j], 0, words[j]) for j in range(wide)]
            words = [jnp.where(coming[j], words[j + q], kept[j]) for j in range(wide - q)] + kept[wide - q:]
            data = [[jnp.where(coming[j], a[j + q], a[j]) for j in range(wide - q)] + a[wide - q:] for a in data]
            step *= 2
        total = total_ref[held]
        for j in range(wide):
            for f in range(3):
                source_ref[f * wide + j, held] = data[f][j]
            source_ref[3 * wide + j, held] = jnp.where(lane8 + j * LANES < total, data[3][j], 0.0)
        return carry

    lax.fori_loop(0, blocks, settle, 0)
    for copy in copies:
        copy.wait()

    sub_row = lax.broadcasted_iota(i32, (SUB, LANES), 0)

    def entries(body):
        return [list_sm[(body + 1) * GROUPS + k] for k in range(GROUPS)]

    def chosen(word, g):
        cell = (word >> 14) & 31
        rows = sub_row + g * SUB
        return cell, [place_ref[t, pl.ds(cell, SUB, stride=0)] == rows for t in range(tiles)]

    def gathered(word, g):
        cell, mask = chosen(word, g)
        for f in range(3):
            value = sum(
                jnp.where(mask[t], own_ref[f * tiles + t, pl.ds(cell, SUB, stride=0)], 0.0) for t in range(tiles)
            )
            yield f, jnp.broadcast_to(jnp.sum(value, axis=1, keepdims=True), (SUB, LANES))

    def gather(body, first, words, held):
        for k, word in enumerate(words):
            for f, value in gathered(word, body * GROUPS + first + k):
                held[3 * k + f] = value

    def scatter(body):
        for k, word in enumerate(entries(body)):
            cell, mask = chosen(word, body * GROUPS + k)
            total = jnp.sum(acc_ref[k], axis=1, keepdims=True)
            for t in range(tiles):
                at = cell * tiles + t
                held = sums_refs[k % len(sums_refs)]
                held[at] = held[at] + jnp.where(mask[t], total, 0.0)

    def part(line, at, ty, tx, tz, acc):
        y, x, z, mass = (source_ref[f * wide + at, pl.ds(line, SUB, stride=0)] for f in range(4))
        dy, dx, dz = y - ty, x - tx, z - tz
        squared = dy * dy + dx * dx + dz * dz
        q = pl.reciprocal(lax.rsqrt(squared))
        outer = jnp.maximum(2.0 - q, 0.0)
        value = jnp.minimum(4.0 - 3.0 * (squared * outer), outer * outer * outer)
        return acc + mass * value

    def compute(targets, k, word, begin, finish, acc):
        line, other = word & 127, (word >> 7) & 127
        offset = jnp.where((word & (1 << 19)) != 0, -4.0, 4.0)
        ty, tx, tz = targets
        moved = tx + offset
        for at in range(begin, finish):
            acc = part(line, at, ty, tx, tz, acc)
            acc = part(other, at, ty, moved, tz, acc)
        acc_ref[k] = acc

    for held in sums_refs:
        held[...] = jnp.zeros(held.shape, f32)
    acc_ref[...] = jnp.zeros(acc_ref.shape, f32)
    bodies = (list_sm[list_tiles * LANES] + (GROUPS - 1)) // GROUPS
    light_bodies = list_sm[list_tiles * LANES + 1] // GROUPS
    gather(0, 0, entries(0)[:half_groups], front_ref)

    def body_step(limit, body, carry):
        words = entries(body)
        scatter(body - 1)
        gather(body, half_groups, words[half_groups:], back_ref)
        zero = jnp.zeros((SUB, LANES), f32)
        for k, word in enumerate(words[:half_groups]):
            compute([front_ref[3 * k + f] for f in range(3)], k, word, 0, limit, zero)
        if limit != small:
            target_ref[:3 * half_groups] = front_ref[...]
            target_ref[3 * half_groups:] = back_ref[...]
        gather(body + 1, 0, entries(body + 1)[:half_groups], front_ref)
        for k, word in enumerate(words[half_groups:]):
            compute([back_ref[3 * k + f] for f in range(3)], half_groups + k, word, 0, limit, zero)
        if limit == small:
            return carry
        flags = words[0]
        for word in words[1:]:
            flags = flags | word

        @pl.when((flags & (1 << 20)) != 0)
        def _():
            def far_step(k, carry):
                word = list_sm[(body + 1) * GROUPS + k]

                @pl.when((word & (1 << 20)) != 0)
                def _():
                    compute([target_ref[3 * k + f] for f in range(3)], k, word, near, wide, acc_ref[k])

                return carry

            lax.fori_loop(0, GROUPS, far_step, 0)

        return carry

    lax.fori_loop(0, light_bodies, functools.partial(body_step, small), 0)
    lax.fori_loop(light_bodies, bodies, functools.partial(body_step, near), 0)
    scatter(bodies - 1)
    for at in range(cells * tiles):
        out_ref[at:at + 1, :] = jnp.sum(sum(held[at] for held in sums_refs), axis=0, keepdims=True) * (16.0 / 3.141592653589793)


def shards(positions, masses, counts, shear_offset):
    cells_y, cells, cells_z, slots = masses.shape
    assert cells_y == 1 and cells_z == 1 and slots % LANES == 0
    tiles = slots // LANES
    rows = cells * tiles
    slot = lax.broadcasted_iota(jnp.int32, (rows, LANES), 1)
    slot = slot + LANES * lax.rem(lax.broadcasted_iota(jnp.int32, (rows, LANES), 0), tiles)
    held = jnp.repeat(counts.reshape(cells), tiles)[:, None]
    weight = jnp.where(slot < held, masses.reshape(rows, LANES), jnp.float32(0.0))
    data = jnp.concatenate([positions.reshape(3, rows, LANES), weight[None]], 0)
    padded = halo(data)
    offset = shear_offset[0]
    shear_index = lax.axis_index("shear")
    cycle = lax.axis_size("shear")
    low = jnp.where(shear_index == 0, offset, 0) % cells
    high = jnp.where(shear_index == cycle - 1, -offset, 0) % cells
    rolls = jnp.stack([low, high]).astype(jnp.int32)

    octants = 2 * len(RODS)
    most_groups = cells * (slots // SUB + octants - 1)
    list_tiles = -(-(most_groups + 3 * GROUPS) // LANES)
    wide = 4 * slots
    smem = pl.BlockSpec(memory_space=pltpu.SMEM)
    vmem = pl.BlockSpec(memory_space=pltpu.VMEM)
    density = pl.pallas_call(
        functools.partial(density_kernel, cells),
        out_shape=jax.ShapeDtypeStruct((rows, LANES), jnp.float32),
        in_specs=[smem, vmem],
        out_specs=vmem,
        scratch_shapes=[
            pltpu.VMEM((9, 4, cells, slots), jnp.float32),
            pltpu.VMEM((4 * wide // LANES, len(RODS) * cells, LANES), jnp.float32),
            pltpu.VMEM((wide // LANES, len(RODS) * cells, LANES), jnp.int32),
            pltpu.VMEM((len(RODS) * cells, LANES), jnp.int32),
            pltpu.VMEM((tiles, cells, LANES), jnp.int32),
            pltpu.VMEM((3 * tiles, cells, LANES), jnp.float32),
            pltpu.VMEM((3 * GROUPS, SUB, LANES), jnp.float32),
            pltpu.VMEM((3 * GROUPS // 2, SUB, LANES), jnp.float32),
            pltpu.VMEM((3 * GROUPS // 2, SUB, LANES), jnp.float32),
            pltpu.VMEM((GROUPS, SUB, LANES), jnp.float32),
            pltpu.VMEM((list_tiles + 1, LANES), jnp.int32),
            pltpu.SMEM(((list_tiles + 1) * LANES,), jnp.int32),
            pltpu.SemaphoreType.DMA((list_tiles + 1,)),
        ] + 4 * [pltpu.VMEM((rows, SUB, LANES), jnp.float32)],
        compiler_params=pltpu.CompilerParams(vmem_limit_bytes=12 * 1024 * 1024),
        name="density",
    )(rolls, padded)
    return density.reshape(masses.shape)


def solution(mesh):
    in_specs = (
        P(None, "shear", None, "cross", None),
        P("shear", None, "cross", None),
        P("shear", None, "cross"),
        P(),
    )
    out_specs = P("shear", None, "cross", None)
    return jax.shard_map(shards, mesh=mesh, in_specs=in_specs, out_specs=out_specs, check_vma=False)
```

```python
import functools
import jax
import jax.numpy as jnp
from jax import lax
from jax.experimental import pallas as pl
from jax.experimental.pallas import tpu as pltpu
from jax.sharding import PartitionSpec as P

LANES = 128
SUB = 8
GROUPS = 16
RODS = ((0, 0), (0, 1), (1, 0), (1, 1))


def halo_kernel(data_ref, out_ref, send_sems, recv_sems, local_sem):
    shear, cross = lax.axis_index("shear"), lax.axis_index("cross")
    rows, planes = lax.axis_size("shear"), lax.axis_size("cross")
    mesh_ids = pl.DeviceIdType.MESH
    along_y = [(lax.rem(shear + rows - step, rows), cross) for step in (-1, 1)]
    along_z = [(shear, lax.rem(cross + planes - step, planes)) for step in (-1, 1)]
    barrier = pltpu.get_barrier_semaphore()
    for device in along_y + along_z:
        pl.semaphore_signal(barrier, inc=1, device_id=device, device_id_type=mesh_ids)
    own = pltpu.make_async_copy(data_ref, out_ref.at[1, 1], local_sem)
    own.start()
    pl.semaphore_wait(barrier, 4)

    def sent(source, y, z, device):
        slot = 3 * y + z
        copy = pltpu.make_async_remote_copy(
            src_ref=source,
            dst_ref=out_ref.at[y, z],
            send_sem=send_sems.at[slot],
            recv_sem=recv_sems.at[slot],
            device_id=device,
            device_id_type=mesh_ids,
        )
        copy.start()
        return copy

    rows_sent = [sent(data_ref, y, 1, along_y[k]) for k, y in enumerate((0, 2))]
    planes_sent = [sent(data_ref, 1, z, along_z[k]) for k, z in enumerate((0, 2))]
    for k, y in enumerate((0, 2)):
        rows_sent[k].wait_recv()
        for j, z in enumerate((0, 2)):
            planes_sent.append(sent(out_ref.at[y, 1], y, z, along_z[j]))
    for copy in rows_sent:
        copy.wait_send()
    for copy in planes_sent:
        copy.wait()
    own.wait()


def halo(data):
    vmem = pl.BlockSpec(memory_space=pltpu.VMEM)
    return pl.pallas_call(
        halo_kernel,
        out_shape=jax.ShapeDtypeStruct((3, 3) + data.shape, data.dtype),
        in_specs=[vmem],
        out_specs=vmem,
        scratch_shapes=[
            pltpu.SemaphoreType.DMA((9,)),
            pltpu.SemaphoreType.DMA((9,)),
            pltpu.SemaphoreType.DMA,
        ],
        compiler_params=pltpu.CompilerParams(
            collective_id=0, has_side_effects=True, vmem_limit_bytes=4 * 1024 * 1024
        ),
        name="halo",
    )(data)


def density_kernel(
    cells, roll_ref, data_ref, out_ref,
    rel_ref, source_ref, move_ref, total_ref, place_ref, own_ref, target_ref, front_ref, back_ref, acc_ref, list_ref, list_sm, list_sem, *sums_refs,
):
    f32, i32 = jnp.float32, jnp.int32
    tiles = data_ref.shape[3] // cells
    slots = tiles * LANES
    wide = 4 * tiles
    list_tiles = list_ref.shape[0] - 1
    limits = tuple(min(wide, wide // 2 + more) for more in (-1, 0, 1))
    half_groups = GROUPS // 2
    half = 0.5

    masks = {}
    for sy in (-1, 0, 1):
        for sz in (-1, 0, 1):
            relation = 3 * (sy + 1) + sz + 1
            parts = []
            for k in range(4):
                value = jnp.concatenate(
                    [data_ref[sy + 1, sz + 1, k, pl.ds(t, cells, stride=tiles), :] for t in range(tiles)], axis=1
                )
                if sy != 0:
                    value = pltpu.roll(value, roll_ref[(sy + 1) // 2], 0)
                parts.append(value)
            y, x, z, mass = parts
            keep = mass > 0.0
            if sy == -1:
                keep = keep & (y >= half)
            elif sy == 1:
                keep = keep & (y <= half)
            if sz == -1:
                keep = keep & (z >= half)
            elif sz == 1:
                keep = keep & (z <= half)
            masks[sy, sz] = keep
            rel_ref[relation, 0] = 4.0 * (y + (sy - half))
            rel_ref[relation, 1] = 4.0 * (x - half)
            rel_ref[relation, 2] = 4.0 * (z + (sz - half))
            rel_ref[relation, 3] = mass
            if sy == 0 and sz == 0:
                own_y, own_x, own_z, own_valid = y, x, z, keep

    octants = []
    for ry, rz in RODS:
        inside = own_valid & ((own_y >= half) if ry else (own_y < half))
        inside = inside & ((own_z >= half) if rz else (own_z < half))
        octants.append(inside & (own_x < half))
        octants.append(inside & (own_x >= half))

    relations = [(sy, sz) for sy in (-1, 0, 1) for sz in (-1, 0, 1)]
    stacked = jnp.concatenate(
        [jnp.where(masks[r], 1.0, 0.0) for r in relations] + [jnp.where(m, 1.0, 0.0) for m in octants], axis=0
    ).astype(jnp.bfloat16)
    row = lax.broadcasted_iota(i32, (slots, slots + LANES), 0)
    col = lax.broadcasted_iota(i32, (slots, slots + LANES), 1)
    triangle = jnp.where((row <= col) | (col >= slots), 1.0, 0.0).astype(jnp.bfloat16)
    ranks = jnp.dot(stacked, triangle, preferred_element_type=f32).astype(i32)

    first = len(relations) * cells
    n_oct = len(octants) * cells
    cell_row = lax.broadcasted_iota(i32, (cells, LANES), 0)
    rods, words, ranking = [], [], []
    for r, (ry, rz) in enumerate(RODS):
        segments = [(0, 0), (2 * ry - 1, 0), (0, 2 * rz - 1), (2 * ry - 1, 2 * rz - 1)]
        starts, start = [], jnp.zeros((cells, LANES), i32)
        for sy, sz in segments:
            at = (3 * (sy + 1) + sz + 1) * cells
            starts.append(start)
            start = start + ranks[at:at + cells, slots:]
        rods.append((segments, starts, start))
        for side in range(2):
            turn = cells - 1 if side else 1
            other = pltpu.roll(cell_row, turn, 0)
            most = jnp.maximum(start, pltpu.roll(start, turn, 0))
            word = (r * cells + cell_row) + ((r * cells + other) << 7) + (cell_row << 14)
            words.append(word + (side << 19) + jnp.where(most > limits[-1] * LANES, 1 << 20, 0))
            ranking.append(sum(jnp.where(most > limit * LANES, n_oct, 0) for limit in limits[:-1]))
    word = jnp.concatenate(words, axis=0).astype(f32)

    totals = ranks[first:, slots:]
    groups = ((totals + (SUB - 1)) >> 3).astype(f32)
    oct_row = lax.broadcasted_iota(i32, (n_oct, LANES), 0)
    oct_lane = lax.broadcasted_iota(i32, (n_oct, LANES), 1)
    light = jnp.concatenate(ranking, axis=0)
    order = (light + oct_row).astype(f32)
    order_lane = jnp.sum(jnp.where(oct_row == oct_lane, order, 0.0), axis=0, keepdims=True)
    lower = jnp.where(order_lane < order, 1.0, 0.0).astype(jnp.bfloat16)
    base = jnp.dot(lower, groups.astype(jnp.bfloat16), preferred_element_type=f32)
    end = base + groups
    place = jnp.full((cells, slots), -1, i32)
    for o, inside in enumerate(octants):
        begin = base[o * cells:(o + 1) * cells].astype(i32)
        begin = jnp.concatenate([begin] * tiles, axis=1)
        rank = ranks[first + o * cells:first + (o + 1) * cells, :slots]
        place = jnp.where(inside, SUB * begin + rank - 1, place)
    for j in range(list_tiles):
        at = (oct_lane + (j * LANES - GROUPS)).astype(f32)
        held = jnp.sum(jnp.where((base <= at) & (at < end), word, 0.0), axis=0, keepdims=True)
        list_ref[j:j + 1, :] = held.astype(i32)
    counted = jnp.zeros((1, LANES), f32)
    for k in range(len(limits)):
        reached = jnp.sum(jnp.where(light <= k * n_oct, groups, 0.0), axis=0, keepdims=True)
        counted = jnp.where(oct_lane[:1] == k, reached, counted)
    list_ref[list_tiles:list_tiles + 1, :] = counted.astype(i32)

    for t in range(tiles):
        lanes = slice(t * LANES, (t + 1) * LANES)
        place_ref[t] = place[:, lanes]
        for f in range(3):
            own_ref[f * tiles + t] = rel_ref[4, f, :, lanes]
    copies = [
        pltpu.make_async_copy(list_ref.at[j], list_sm.at[pl.ds(j * LANES, LANES)], list_sem.at[j])
        for j in range(list_tiles + 1)
    ]
    lane = lax.broadcasted_iota(i32, (cells, LANES), 1)
    for r, (segments, starts, total) in enumerate(rods):
        held = slice(r * cells, (r + 1) * cells)
        total_ref[held] = total
        for k, (sy, sz) in enumerate(segments):
            at = (3 * (sy + 1) + sz + 1) * cells
            for t in range(tiles):
                lanes = slice(t * LANES, (t + 1) * LANES)
                word = lane << 10
                if k > 0:
                    shift = (k * slots + t * LANES + 1) + lane - starts[k] - ranks[at:at + cells, lanes]
                    word = word + jnp.where(masks[sy, sz][:, lanes], shift, 0)
                move_ref[k * tiles + t, held] = word
    for copy in copies:
        copy.start()

    lane8 = lax.broadcasted_iota(i32, (SUB, LANES), 1)
    blocks = len(RODS) * cells // SUB

    def ranked(words):
        step = 1
        while step < LANES:
            inner = lane8 < LANES - step
            turned = [pltpu.roll(w, LANES - step, 1) for w in words] + [jnp.zeros_like(lane8)]
            coming = [jnp.where(inner, turned[j], turned[j + 1]) for j in range(len(words))]
            words = [
                jnp.where((c & step) != 0, c, jnp.where((w & step) != 0, 0, w)) for c, w in zip(coming, words)
            ]
            step *= 2
        return words

    def settle(block):
        rod = block // (cells // SUB)
        top = pl.multiple_of((block - rod * (cells // SUB)) * SUB, SUB)
        held = pl.ds(pl.multiple_of(block * SUB, SUB), SUB)
        ry, rz = 2 * (rod >> 1), 2 * (rod & 1)
        segments = [4, 3 * ry + 1, 3 + rz, 3 * ry + rz]
        words = [move_ref[j, held] for j in range(wide)]
        words = words[:tiles - 1] + ranked(words[tiles - 1:])
        origin = [w >> 10 for w in words]
        raw = [
            [
                rel_ref[segments[j // tiles], f, pl.ds(top, SUB), (j % tiles) * LANES:(j % tiles + 1) * LANES]
                for j in range(wide)
            ]
            for f in range(4)
        ]
        data = [[] for _ in range(4)]
        for j in range(wide):
            for f in range(4):
                here = raw[f][j]
                if j >= tiles:
                    here = jnp.take_along_axis(here, origin[j], axis=1, mode="promise_in_bounds")
                if tiles - 1 <= j < wide - 1:
                    after = jnp.take_along_axis(raw[f][j + 1], origin[j], axis=1, mode="promise_in_bounds")
                    here = jnp.where(origin[j] >= lane8, here, after)
                data[f].append(here)
        step = LANES
        while step < wide * LANES:
            q = step // LANES
            coming = [(w & step) != 0 for w in words[q:]]
            leaving = [(w & step) != 0 for w in words]
            kept = [jnp.where(leaving[j], 0, words[j]) for j in range(wide)]
            words = [jnp.where(coming[j], words[j + q], kept[j]) for j in range(wide - q)] + kept[wide - q:]
            data = [[jnp.where(coming[j], a[j + q], a[j]) for j in range(wide - q)] + a[wide - q:] for a in data]
            step *= 2
        total = total_ref[held]
        for j in range(wide):
            for f in range(3):
                source_ref[f * wide + j, held] = data[f][j]
            source_ref[3 * wide + j, held] = jnp.where(lane8 + j * LANES < total, data[3][j], 0.0)

    together = next(n for n in (4, 2, 1) if blocks % n == 0)

    def settle_some(step, carry):
        for k in range(together):
            settle(step * together + k)
        return carry

    lax.fori_loop(0, blocks // together, settle_some, 0)
    for copy in copies:
        copy.wait()

    sub_row = lax.broadcasted_iota(i32, (SUB, LANES), 0)

    def entries(body):
        return [list_sm[(body + 1) * GROUPS + k] for k in range(GROUPS)]

    def chosen(word, g):
        cell = (word >> 14) & 31
        rows = sub_row + g * SUB
        return cell, [place_ref[t, pl.ds(cell, SUB, stride=0)] == rows for t in range(tiles)]

    def gathered(word, g):
        cell, mask = chosen(word, g)
        for f in range(3):
            value = sum(
                jnp.where(mask[t], own_ref[f * tiles + t, pl.ds(cell, SUB, stride=0)], 0.0) for t in range(tiles)
            )
            yield f, jnp.broadcast_to(jnp.sum(value, axis=1, keepdims=True), (SUB, LANES))

    def gather(body, first, words, held):
        for k, word in enumerate(words):
            for f, value in gathered(word, body * GROUPS + first + k):
                held[3 * k + f] = value

    def scatter(body):
        for k, word in enumerate(entries(body)):
            cell, mask = chosen(word, body * GROUPS + k)
            total = jnp.sum(acc_ref[k], axis=1, keepdims=True)
            for t in range(tiles):
                at = cell * tiles + t
                held = sums_refs[k % len(sums_refs)]
                held[at] = held[at] + jnp.where(mask[t], total, 0.0)

    def part(line, at, ty, tx, tz, acc):
        y, x, z, mass = (source_ref[f * wide + at, pl.ds(line, SUB, stride=0)] for f in range(4))
        dy, dx, dz = y - ty, x - tx, z - tz
        squared = dy * dy + dx * dx + dz * dz
        q = pl.reciprocal(lax.rsqrt(squared))
        outer = jnp.maximum(2.0 - q, 0.0)
        value = jnp.minimum(4.0 - 3.0 * (squared * outer), outer * outer * outer)
        return acc + mass * value

    def compute(targets, k, word, begin, finish, acc):
        line, other = word & 127, (word >> 7) & 127
        offset = jnp.where((word & (1 << 19)) != 0, -4.0, 4.0)
        ty, tx, tz = targets
        moved = tx + offset
        for at in range(begin, finish):
            acc = part(line, at, ty, tx, tz, acc)
            acc = part(other, at, ty, moved, tz, acc)
        acc_ref[k] = acc

    for held in sums_refs:
        held[...] = jnp.zeros(held.shape, f32)
    acc_ref[...] = jnp.zeros(acc_ref.shape, f32)
    reached = [list_sm[list_tiles * LANES + k] for k in range(len(limits))]
    bodies = (reached[-1] + (GROUPS - 1)) // GROUPS
    bounds = [0] + [n // GROUPS for n in reached[:-1]] + [bodies]
    gather(0, 0, entries(0)[:half_groups], front_ref)

    def body_step(limit, body, carry):
        words = entries(body)
        scatter(body - 1)
        gather(body, half_groups, words[half_groups:], back_ref)
        zero = jnp.zeros((SUB, LANES), f32)
        for k, word in enumerate(words[:half_groups]):
            compute([front_ref[3 * k + f] for f in range(3)], k, word, 0, limit, zero)
        if limit == limits[-1]:
            target_ref[:3 * half_groups] = front_ref[...]
            target_ref[3 * half_groups:] = back_ref[...]
        gather(body + 1, 0, entries(body + 1)[:half_groups], front_ref)
        for k, word in enumerate(words[half_groups:]):
            compute([back_ref[3 * k + f] for f in range(3)], half_groups + k, word, 0, limit, zero)
        if limit != limits[-1]:
            return carry
        flags = words[0]
        for word in words[1:]:
            flags = flags | word

        @pl.when((flags & (1 << 20)) != 0)
        def _():
            def far_step(k, carry):
                word = list_sm[(body + 1) * GROUPS + k]

                @pl.when((word & (1 << 20)) != 0)
                def _():
                    compute([target_ref[3 * k + f] for f in range(3)], k, word, limit, wide, acc_ref[k])

                return carry

            lax.fori_loop(0, GROUPS, far_step, 0)

        return carry

    for limit, begin, finish in zip(limits, bounds, bounds[1:]):
        lax.fori_loop(begin, finish, functools.partial(body_step, limit), 0)
    scatter(bodies - 1)
    for at in range(cells * tiles):
        out_ref[at:at + 1, :] = jnp.sum(sum(held[at] for held in sums_refs), axis=0, keepdims=True) * (16.0 / 3.141592653589793)


def shards(positions, masses, counts, shear_offset):
    cells_y, cells, cells_z, slots = masses.shape
    assert cells_y == 1 and cells_z == 1 and slots % LANES == 0
    tiles = slots // LANES
    rows = cells * tiles
    slot = lax.broadcasted_iota(jnp.int32, (rows, LANES), 1)
    slot = slot + LANES * lax.rem(lax.broadcasted_iota(jnp.int32, (rows, LANES), 0), tiles)
    held = jnp.repeat(counts.reshape(cells), tiles)[:, None]
    weight = jnp.where(slot < held, masses.reshape(rows, LANES), jnp.float32(0.0))
    data = jnp.concatenate([positions.reshape(3, rows, LANES), weight[None]], 0)
    padded = halo(data)
    offset = shear_offset[0]
    shear_index = lax.axis_index("shear")
    cycle = lax.axis_size("shear")
    low = jnp.where(shear_index == 0, offset, 0) % cells
    high = jnp.where(shear_index == cycle - 1, -offset, 0) % cells
    rolls = jnp.stack([low, high]).astype(jnp.int32)

    octants = 2 * len(RODS)
    most_groups = cells * (slots // SUB + octants - 1)
    list_tiles = -(-(most_groups + 3 * GROUPS) // LANES)
    wide = 4 * slots
    smem = pl.BlockSpec(memory_space=pltpu.SMEM)
    vmem = pl.BlockSpec(memory_space=pltpu.VMEM)
    density = pl.pallas_call(
        functools.partial(density_kernel, cells),
        out_shape=jax.ShapeDtypeStruct((rows, LANES), jnp.float32),
        in_specs=[smem, vmem],
        out_specs=vmem,
        scratch_shapes=[
            pltpu.VMEM((9, 4, cells, slots), jnp.float32),
            pltpu.VMEM((4 * wide // LANES, len(RODS) * cells, LANES), jnp.float32),
            pltpu.VMEM((wide // LANES, len(RODS) * cells, LANES), jnp.int32),
            pltpu.VMEM((len(RODS) * cells, LANES), jnp.int32),
            pltpu.VMEM((tiles, cells, LANES), jnp.int32),
            pltpu.VMEM((3 * tiles, cells, LANES), jnp.float32),
            pltpu.VMEM((3 * GROUPS, SUB, LANES), jnp.float32),
            pltpu.VMEM((3 * GROUPS // 2, SUB, LANES), jnp.float32),
            pltpu.VMEM((3 * GROUPS // 2, SUB, LANES), jnp.float32),
            pltpu.VMEM((GROUPS, SUB, LANES), jnp.float32),
            pltpu.VMEM((list_tiles + 1, LANES), jnp.int32),
            pltpu.SMEM(((list_tiles + 1) * LANES,), jnp.int32),
            pltpu.SemaphoreType.DMA((list_tiles + 1,)),
        ] + 4 * [pltpu.VMEM((rows, SUB, LANES), jnp.float32)],
        compiler_params=pltpu.CompilerParams(vmem_limit_bytes=12 * 1024 * 1024),
        name="density",
    )(rolls, padded)
    return density.reshape(masses.shape)


def solution(mesh):
    in_specs = (
        P(None, "shear", None, "cross", None),
        P("shear", None, "cross", None),
        P("shear", None, "cross"),
        P(),
    )
    out_specs = P("shear", None, "cross", None)
    return jax.shard_map(shards, mesh=mesh, in_specs=in_specs, out_specs=out_specs, check_vma=False)
```

```python
import functools
import jax
import jax.numpy as jnp
from jax import lax
from jax.experimental import pallas as pl
from jax.experimental.pallas import tpu as pltpu
from jax.sharding import PartitionSpec as P

LANES = 128
SUB = 8
GROUPS = 16
RODS = ((0, 0), (0, 1), (1, 0), (1, 1))


def halo_kernel(
    pos_ref, mass_ref, counts_ref, out_ref, held_ref, counts_sm, send_sems, recv_sems, local_sems,
):
    shear, cross = lax.axis_index("shear"), lax.axis_index("cross")
    rows, planes = lax.axis_size("shear"), lax.axis_size("cross")
    mesh_ids = pl.DeviceIdType.MESH
    sides = (0, 2) if planes > 2 else (0,)
    along_y = [(lax.rem(shear + rows - step, rows), cross) for step in (-1, 1)]
    along_z = [(shear, lax.rem(cross + planes - step, planes)) for step in (-1, 1)][:len(sides)]
    barrier = pltpu.get_barrier_semaphore()
    for device in along_y + along_z:
        pl.semaphore_signal(barrier, inc=1, device_id=device, device_id_type=mesh_ids)
    own = out_ref.at[1, 1]
    loads = [
        pltpu.make_async_copy(counts_ref, counts_sm, local_sems.at[0]),
        pltpu.make_async_copy(mass_ref, held_ref, local_sems.at[1]),
        pltpu.make_async_copy(pos_ref, own.at[pl.ds(0, 3)], local_sems.at[2]),
    ]
    for copy in loads:
        copy.start()
    for copy in loads[:2]:
        copy.wait()
    lines, cells = held_ref.shape[0], counts_sm.shape[0]
    tiles = lines // cells
    line = lax.broadcasted_iota(jnp.int32, (lines, LANES), 0)
    slot = lax.broadcasted_iota(jnp.int32, (lines, LANES), 1) + LANES * lax.rem(line, tiles)
    limit = jnp.zeros((lines, LANES), jnp.int32)
    for cell in range(cells):
        inside = (line >= cell * tiles) & (line < (cell + 1) * tiles)
        limit = jnp.where(inside, counts_sm[cell], limit)
    own[3] = jnp.where(slot < limit, held_ref[...], 0.0)
    loads[2].wait()
    pl.semaphore_wait(barrier, len(along_y) + len(along_z))

    def sent(source, y, z, device):
        at = 3 * y + z
        copy = pltpu.make_async_remote_copy(
            src_ref=source,
            dst_ref=out_ref.at[y, z],
            send_sem=send_sems.at[at],
            recv_sem=recv_sems.at[at],
            device_id=device,
            device_id_type=mesh_ids,
        )
        copy.start()
        return copy

    rows_sent = [sent(own, y, 1, along_y[k]) for k, y in enumerate((0, 2))]
    planes_sent = [sent(own, 1, z, along_z[k]) for k, z in enumerate(sides)]
    for k, y in enumerate((0, 2)):
        rows_sent[k].wait_recv()
        for j, z in enumerate(sides):
            planes_sent.append(sent(out_ref.at[y, 1], y, z, along_z[j]))
    for copy in rows_sent:
        copy.wait_send()
    for copy in planes_sent:
        copy.wait()


def halo(positions, masses, counts):
    lines = masses.shape[0]
    depth = 3 if lax.axis_size("cross") > 2 else 2
    return pl.pallas_call(
        halo_kernel,
        out_shape=jax.ShapeDtypeStruct((3, depth, 4, lines, LANES), masses.dtype),
        in_specs=[pl.BlockSpec(memory_space=pl.ANY)] * 3,
        out_specs=pl.BlockSpec(memory_space=pltpu.VMEM),
        scratch_shapes=[
            pltpu.VMEM((lines, LANES), jnp.float32),
            pltpu.SMEM(counts.shape, jnp.int32),
            pltpu.SemaphoreType.DMA((9,)),
            pltpu.SemaphoreType.DMA((9,)),
            pltpu.SemaphoreType.DMA((3,)),
        ],
        compiler_params=pltpu.CompilerParams(
            collective_id=0, has_side_effects=True, vmem_limit_bytes=4 * 1024 * 1024
        ),
        name="halo",
    )(positions, masses, counts)


def density_kernel(
    cells, roll_ref, data_ref, out_ref,
    rel_ref, source_ref, move_ref, total_ref, place_ref, own_ref, target_ref, front_ref, back_ref, acc_ref, list_ref, list_sm, list_sem, *sums_refs,
):
    f32, i32 = jnp.float32, jnp.int32
    tiles = data_ref.shape[3] // cells
    slots = tiles * LANES
    wide = 4 * tiles
    list_tiles = list_ref.shape[0] - 1
    limits = tuple(min(wide, wide // 2 + more) for more in (-1, 0, 1))
    half_groups = GROUPS // 2
    half = 0.5

    masks = {}
    for sy in (-1, 0, 1):
        for sz in (-1, 0, 1):
            relation = 3 * (sy + 1) + sz + 1
            plane = sz + 1 if data_ref.shape[1] > 2 else 1 - abs(sz)
            parts = []
            for k in range(4):
                value = jnp.concatenate(
                    [data_ref[sy + 1, plane, k, pl.ds(t, cells, stride=tiles), :] for t in range(tiles)], axis=1
                )
                if sy != 0:
                    value = pltpu.roll(value, roll_ref[(sy + 1) // 2], 0)
                parts.append(value)
            y, x, z, mass = parts
            keep = mass > 0.0
            if sy == -1:
                keep = keep & (y >= half)
            elif sy == 1:
                keep = keep & (y <= half)
            if sz == -1:
                keep = keep & (z >= half)
            elif sz == 1:
                keep = keep & (z <= half)
            masks[sy, sz] = keep
            rel_ref[relation, 0] = 4.0 * (y + (sy - half))
            rel_ref[relation, 1] = 4.0 * (x - half)
            rel_ref[relation, 2] = 4.0 * (z + (sz - half))
            rel_ref[relation, 3] = mass
            if sy == 0 and sz == 0:
                own_y, own_x, own_z, own_valid = y, x, z, keep

    octants = []
    for ry, rz in RODS:
        inside = own_valid & ((own_y >= half) if ry else (own_y < half))
        inside = inside & ((own_z >= half) if rz else (own_z < half))
        octants.append(inside & (own_x < half))
        octants.append(inside & (own_x >= half))

    relations = [(sy, sz) for sy in (-1, 0, 1) for sz in (-1, 0, 1)]
    stacked = jnp.concatenate(
        [jnp.where(masks[r], 1.0, 0.0) for r in relations] + [jnp.where(m, 1.0, 0.0) for m in octants], axis=0
    ).astype(jnp.bfloat16)
    row = lax.broadcasted_iota(i32, (slots, slots + LANES), 0)
    col = lax.broadcasted_iota(i32, (slots, slots + LANES), 1)
    triangle = jnp.where((row <= col) | (col >= slots), 1.0, 0.0).astype(jnp.bfloat16)
    ranks = jnp.dot(stacked, triangle, preferred_element_type=f32).astype(i32)

    first = len(relations) * cells
    n_oct = len(octants) * cells
    cell_row = lax.broadcasted_iota(i32, (cells, LANES), 0)
    rods, words, ranking = [], [], []
    for r, (ry, rz) in enumerate(RODS):
        segments = [(0, 0), (2 * ry - 1, 0), (0, 2 * rz - 1), (2 * ry - 1, 2 * rz - 1)]
        starts, start = [], jnp.zeros((cells, LANES), i32)
        for sy, sz in segments:
            at = (3 * (sy + 1) + sz + 1) * cells
            starts.append(start)
            start = start + ranks[at:at + cells, slots:]
        rods.append((segments, starts, start))
        for side in range(2):
            turn = cells - 1 if side else 1
            other = pltpu.roll(cell_row, turn, 0)
            most = jnp.maximum(start, pltpu.roll(start, turn, 0))
            word = (r * cells + cell_row) + ((r * cells + other) << 7) + (cell_row << 14)
            words.append(word + (side << 19) + jnp.where(most > limits[-1] * LANES, 1 << 20, 0))
            ranking.append(sum(jnp.where(most > limit * LANES, n_oct, 0) for limit in limits[:-1]))
    word = jnp.concatenate(words, axis=0).astype(f32)

    totals = ranks[first:, slots:]
    groups = ((totals + (SUB - 1)) >> 3).astype(f32)
    oct_row = lax.broadcasted_iota(i32, (n_oct, LANES), 0)
    oct_lane = lax.broadcasted_iota(i32, (n_oct, LANES), 1)
    light = jnp.concatenate(ranking, axis=0)
    order = (light + oct_row).astype(f32)
    order_lane = jnp.sum(jnp.where(oct_row == oct_lane, order, 0.0), axis=0, keepdims=True)
    lower = jnp.where(order_lane < order, 1.0, 0.0).astype(jnp.bfloat16)
    base = jnp.dot(lower, groups.astype(jnp.bfloat16), preferred_element_type=f32)
    end = base + groups
    place = jnp.full((cells, slots), -1, i32)
    for o, inside in enumerate(octants):
        begin = base[o * cells:(o + 1) * cells].astype(i32)
        begin = jnp.concatenate([begin] * tiles, axis=1)
        rank = ranks[first + o * cells:first + (o + 1) * cells, :slots]
        place = jnp.where(inside, SUB * begin + rank - 1, place)
    for j in range(list_tiles):
        at = (oct_lane + (j * LANES - GROUPS)).astype(f32)
        held = jnp.sum(jnp.where((base <= at) & (at < end), word, 0.0), axis=0, keepdims=True)
        list_ref[j:j + 1, :] = held.astype(i32)
    counted = jnp.zeros((1, LANES), f32)
    for k in range(len(limits)):
        reached = jnp.sum(jnp.where(light <= k * n_oct, groups, 0.0), axis=0, keepdims=True)
        counted = jnp.where(oct_lane[:1] == k, reached, counted)
    list_ref[list_tiles:list_tiles + 1, :] = counted.astype(i32)

    for t in range(tiles):
        lanes = slice(t * LANES, (t + 1) * LANES)
        place_ref[t] = place[:, lanes]
        for f in range(3):
            own_ref[f * tiles + t] = rel_ref[4, f, :, lanes]
    copies = [
        pltpu.make_async_copy(list_ref.at[j], list_sm.at[pl.ds(j * LANES, LANES)], list_sem.at[j])
        for j in range(list_tiles + 1)
    ]
    lane = lax.broadcasted_iota(i32, (cells, LANES), 1)
    for r, (segments, starts, total) in enumerate(rods):
        held = slice(r * cells, (r + 1) * cells)
        total_ref[held] = total
        for k, (sy, sz) in enumerate(segments):
            at = (3 * (sy + 1) + sz + 1) * cells
            for t in range(tiles):
                lanes = slice(t * LANES, (t + 1) * LANES)
                word = lane << 10
                if k > 0:
                    shift = (k * slots + t * LANES + 1) + lane - starts[k] - ranks[at:at + cells, lanes]
                    word = word + jnp.where(masks[sy, sz][:, lanes], shift, 0)
                move_ref[k * tiles + t, held] = word
    for copy in copies:
        copy.start()

    lane8 = lax.broadcasted_iota(i32, (SUB, LANES), 1)
    blocks = len(RODS) * cells // SUB

    def ranked(words):
        step = 1
        while step < LANES:
            inner = lane8 < LANES - step
            turned = [pltpu.roll(w, LANES - step, 1) for w in words] + [jnp.zeros_like(lane8)]
            coming = [jnp.where(inner, turned[j], turned[j + 1]) for j in range(len(words))]
            words = [
                jnp.where((c & step) != 0, c, jnp.where((w & step) != 0, 0, w)) for c, w in zip(coming, words)
            ]
            step *= 2
        return words

    def settle(block):
        rod = block // (cells // SUB)
        top = pl.multiple_of((block - rod * (cells // SUB)) * SUB, SUB)
        held = pl.ds(pl.multiple_of(block * SUB, SUB), SUB)
        ry, rz = 2 * (rod >> 1), 2 * (rod & 1)
        segments = [4, 3 * ry + 1, 3 + rz, 3 * ry + rz]
        words = [move_ref[j, held] for j in range(wide)]
        words = words[:tiles - 1] + ranked(words[tiles - 1:])
        origin = [w >> 10 for w in words]
        raw = [
            [
                rel_ref[segments[j // tiles], f, pl.ds(top, SUB), (j % tiles) * LANES:(j % tiles + 1) * LANES]
                for j in range(wide)
            ]
            for f in range(4)
        ]
        data = [[] for _ in range(4)]
        for j in range(wide):
            for f in range(4):
                here = raw[f][j]
                if j >= tiles:
                    here = jnp.take_along_axis(here, origin[j], axis=1, mode="promise_in_bounds")
                if tiles - 1 <= j < wide - 1:
                    after = jnp.take_along_axis(raw[f][j + 1], origin[j], axis=1, mode="promise_in_bounds")
                    here = jnp.where(origin[j] >= lane8, here, after)
                data[f].append(here)
        step = LANES
        while step < wide * LANES:
            q = step // LANES
            coming = [(w & step) != 0 for w in words[q:]]
            leaving = [(w & step) != 0 for w in words]
            kept = [jnp.where(leaving[j], 0, words[j]) for j in range(wide)]
            words = [jnp.where(coming[j], words[j + q], kept[j]) for j in range(wide - q)] + kept[wide - q:]
            data = [[jnp.where(coming[j], a[j + q], a[j]) for j in range(wide - q)] + a[wide - q:] for a in data]
            step *= 2
        total = total_ref[held]
        for j in range(wide):
            for f in range(3):
                source_ref[f * wide + j, held] = data[f][j]
            source_ref[3 * wide + j, held] = jnp.where(lane8 + j * LANES < total, data[3][j], 0.0)

    together = next(n for n in (4, 2, 1) if blocks % n == 0)

    def settle_some(step, carry):
        for k in range(together):
            settle(step * together + k)
        return carry

    lax.fori_loop(0, blocks // together, settle_some, 0)
    for copy in copies:
        copy.wait()

    sub_row = lax.broadcasted_iota(i32, (SUB, LANES), 0)

    def entries(body):
        return [list_sm[(body + 1) * GROUPS + k] for k in range(GROUPS)]

    def chosen(word, g):
        cell = (word >> 14) & 31
        rows = sub_row + g * SUB
        return cell, [place_ref[t, pl.ds(cell, SUB, stride=0)] == rows for t in range(tiles)]

    def gathered(word, g):
        cell, mask = chosen(word, g)
        for f in range(3):
            value = sum(
                jnp.where(mask[t], own_ref[f * tiles + t, pl.ds(cell, SUB, stride=0)], 0.0) for t in range(tiles)
            )
            yield f, jnp.broadcast_to(jnp.sum(value, axis=1, keepdims=True), (SUB, LANES))

    def gather(body, first, words, held):
        for k, word in enumerate(words):
            for f, value in gathered(word, body * GROUPS + first + k):
                held[3 * k + f] = value

    def scatter(body):
        for k, word in enumerate(entries(body)):
            cell, mask = chosen(word, body * GROUPS + k)
            total = jnp.sum(acc_ref[k], axis=1, keepdims=True)
            for t in range(tiles):
                at = cell * tiles + t
                held = sums_refs[k % len(sums_refs)]
                held[at] = held[at] + jnp.where(mask[t], total, 0.0)

    def part(line, at, ty, tx, tz, acc):
        y, x, z, mass = (source_ref[f * wide + at, pl.ds(line, SUB, stride=0)] for f in range(4))
        dy, dx, dz = y - ty, x - tx, z - tz
        squared = dy * dy + dx * dx + dz * dz
        q = pl.reciprocal(lax.rsqrt(squared))
        outer = jnp.maximum(2.0 - q, 0.0)
        value = jnp.minimum(4.0 - 3.0 * (squared * outer), outer * outer * outer)
        return acc + mass * value

    def compute(targets, k, word, begin, finish, acc):
        line, other = word & 127, (word >> 7) & 127
        offset = jnp.where((word & (1 << 19)) != 0, -4.0, 4.0)
        ty, tx, tz = targets
        moved = tx + offset
        for at in range(begin, finish):
            acc = part(line, at, ty, tx, tz, acc)
            acc = part(other, at, ty, moved, tz, acc)
        acc_ref[k] = acc

    for held in sums_refs:
        held[...] = jnp.zeros(held.shape, f32)
    acc_ref[...] = jnp.zeros(acc_ref.shape, f32)
    reached = [list_sm[list_tiles * LANES + k] for k in range(len(limits))]
    bodies = (reached[-1] + (GROUPS - 1)) // GROUPS
    bounds = [0] + [n // GROUPS for n in reached[:-1]] + [bodies]
    gather(0, 0, entries(0)[:half_groups], front_ref)

    def body_step(limit, body, carry):
        words = entries(body)
        scatter(body - 1)
        gather(body, half_groups, words[half_groups:], back_ref)
        zero = jnp.zeros((SUB, LANES), f32)
        for k, word in enumerate(words[:half_groups]):
            compute([front_ref[3 * k + f] for f in range(3)], k, word, 0, limit, zero)
        if limit == limits[-1]:
            target_ref[:3 * half_groups] = front_ref[...]
            target_ref[3 * half_groups:] = back_ref[...]
        gather(body + 1, 0, entries(body + 1)[:half_groups], front_ref)
        for k, word in enumerate(words[half_groups:]):
            compute([back_ref[3 * k + f] for f in range(3)], half_groups + k, word, 0, limit, zero)
        if limit != limits[-1]:
            return carry
        flags = words[0]
        for word in words[1:]:
            flags = flags | word

        @pl.when((flags & (1 << 20)) != 0)
        def _():
            def far_step(k, carry):
                word = list_sm[(body + 1) * GROUPS + k]

                @pl.when((word & (1 << 20)) != 0)
                def _():
                    compute([target_ref[3 * k + f] for f in range(3)], k, word, limit, wide, acc_ref[k])

                return carry

            lax.fori_loop(0, GROUPS, far_step, 0)

        return carry

    for limit, begin, finish in zip(limits, bounds, bounds[1:]):
        lax.fori_loop(begin, finish, functools.partial(body_step, limit), 0)
    scatter(bodies - 1)
    for at in range(cells * tiles):
        out_ref[at:at + 1, :] = jnp.sum(sum(held[at] for held in sums_refs), axis=0, keepdims=True) * (16.0 / 3.141592653589793)


def shards(positions, masses, counts, shear_offset):
    cells_y, cells, cells_z, slots = masses.shape
    assert cells_y == 1 and cells_z == 1 and slots % LANES == 0
    tiles = slots // LANES
    rows = cells * tiles
    padded = halo(positions.reshape(3, rows, LANES), masses.reshape(rows, LANES), counts.reshape(cells))
    offset = shear_offset[0]
    shear_index = lax.axis_index("shear")
    cycle = lax.axis_size("shear")
    low = jnp.where(shear_index == 0, offset, 0) % cells
    high = jnp.where(shear_index == cycle - 1, -offset, 0) % cells
    rolls = jnp.stack([low, high]).astype(jnp.int32)

    octants = 2 * len(RODS)
    most_groups = cells * (slots // SUB + octants - 1)
    list_tiles = -(-(most_groups + 3 * GROUPS) // LANES)
    wide = 4 * slots
    smem = pl.BlockSpec(memory_space=pltpu.SMEM)
    vmem = pl.BlockSpec(memory_space=pltpu.VMEM)
    density = pl.pallas_call(
        functools.partial(density_kernel, cells),
        out_shape=jax.ShapeDtypeStruct((rows, LANES), jnp.float32),
        in_specs=[smem, vmem],
        out_specs=vmem,
        scratch_shapes=[
            pltpu.VMEM((9, 4, cells, slots), jnp.float32),
            pltpu.VMEM((4 * wide // LANES, len(RODS) * cells, LANES), jnp.float32),
            pltpu.VMEM((wide // LANES, len(RODS) * cells, LANES), jnp.int32),
            pltpu.VMEM((len(RODS) * cells, LANES), jnp.int32),
            pltpu.VMEM((tiles, cells, LANES), jnp.int32),
            pltpu.VMEM((3 * tiles, cells, LANES), jnp.float32),
            pltpu.VMEM((3 * GROUPS, SUB, LANES), jnp.float32),
            pltpu.VMEM((3 * GROUPS // 2, SUB, LANES), jnp.float32),
            pltpu.VMEM((3 * GROUPS // 2, SUB, LANES), jnp.float32),
            pltpu.VMEM((GROUPS, SUB, LANES), jnp.float32),
            pltpu.VMEM((list_tiles + 1, LANES), jnp.int32),
            pltpu.SMEM(((list_tiles + 1) * LANES,), jnp.int32),
            pltpu.SemaphoreType.DMA((list_tiles + 1,)),
        ] + 4 * [pltpu.VMEM((rows, SUB, LANES), jnp.float32)],
        compiler_params=pltpu.CompilerParams(vmem_limit_bytes=12 * 1024 * 1024),
        name="density",
    )(rolls, padded)
    return density.reshape(masses.shape)


def solution(mesh):
    in_specs = (
        P(None, "shear", None, "cross", None),
        P("shear", None, "cross", None),
        P("shear", None, "cross"),
        P(),
    )
    out_specs = P("shear", None, "cross", None)
    return jax.shard_map(shards, mesh=mesh, in_specs=in_specs, out_specs=out_specs, check_vma=False)
```

```python
import functools
import jax
import jax.numpy as jnp
from jax import lax
from jax.experimental import pallas as pl
from jax.experimental.pallas import tpu as pltpu
from jax.sharding import PartitionSpec as P

LANES = 128
SUB = 8
GROUPS = 8
RODS = ((0, 0), (0, 1), (1, 0), (1, 1))


def halo_kernel(
    pos_ref, mass_ref, counts_ref, out_ref, held_ref, counts_sm, send_sems, recv_sems, local_sems,
):
    shear, cross = lax.axis_index("shear"), lax.axis_index("cross")
    rows, planes = lax.axis_size("shear"), lax.axis_size("cross")
    mesh_ids = pl.DeviceIdType.MESH
    sides = (0, 2) if planes > 2 else (0,)
    along_y = [(lax.rem(shear + rows - step, rows), cross) for step in (-1, 1)]
    along_z = [(shear, lax.rem(cross + planes - step, planes)) for step in (-1, 1)][:len(sides)]
    barrier = pltpu.get_barrier_semaphore()
    for device in along_y + along_z:
        pl.semaphore_signal(barrier, inc=1, device_id=device, device_id_type=mesh_ids)
    own = out_ref.at[1, 1]
    loads = [
        pltpu.make_async_copy(counts_ref, counts_sm, local_sems.at[0]),
        pltpu.make_async_copy(mass_ref, held_ref, local_sems.at[1]),
        pltpu.make_async_copy(pos_ref, own.at[pl.ds(0, 3)], local_sems.at[2]),
    ]
    for copy in loads:
        copy.start()
    for copy in loads[:2]:
        copy.wait()
    lines, cells = held_ref.shape[0], counts_sm.shape[0]
    tiles = lines // cells
    line = lax.broadcasted_iota(jnp.int32, (lines, LANES), 0)
    slot = lax.broadcasted_iota(jnp.int32, (lines, LANES), 1) + LANES * lax.rem(line, tiles)
    limit = jnp.zeros((lines, LANES), jnp.int32)
    for cell in range(cells):
        inside = (line >= cell * tiles) & (line < (cell + 1) * tiles)
        limit = jnp.where(inside, counts_sm[cell], limit)
    own[3] = jnp.where(slot < limit, held_ref[...], 0.0)
    loads[2].wait()
    pl.semaphore_wait(barrier, len(along_y) + len(along_z))

    def sent(source, y, z, device):
        at = 3 * y + z
        copy = pltpu.make_async_remote_copy(
            src_ref=source,
            dst_ref=out_ref.at[y, z],
            send_sem=send_sems.at[at],
            recv_sem=recv_sems.at[at],
            device_id=device,
            device_id_type=mesh_ids,
        )
        copy.start()
        return copy

    rows_sent = [sent(own, y, 1, along_y[k]) for k, y in enumerate((0, 2))]
    planes_sent = [sent(own, 1, z, along_z[k]) for k, z in enumerate(sides)]
    for k, y in ((1, 2), (0, 0)):
        rows_sent[k].wait_recv()
        for j, z in enumerate(sides):
            planes_sent.append(sent(out_ref.at[y, 1], y, z, along_z[j]))
    for copy in rows_sent:
        copy.wait_send()
    for copy in planes_sent:
        copy.wait()


def halo(positions, masses, counts):
    lines = masses.shape[0]
    depth = 3 if lax.axis_size("cross") > 2 else 2
    return pl.pallas_call(
        halo_kernel,
        out_shape=jax.ShapeDtypeStruct((3, depth, 4, lines, LANES), masses.dtype),
        in_specs=[pl.BlockSpec(memory_space=pl.ANY)] * 3,
        out_specs=pl.BlockSpec(memory_space=pltpu.VMEM),
        scratch_shapes=[
            pltpu.VMEM((lines, LANES), jnp.float32),
            pltpu.SMEM(counts.shape, jnp.int32),
            pltpu.SemaphoreType.DMA((9,)),
            pltpu.SemaphoreType.DMA((9,)),
            pltpu.SemaphoreType.DMA((3,)),
        ],
        compiler_params=pltpu.CompilerParams(
            collective_id=0, has_side_effects=True, vmem_limit_bytes=4 * 1024 * 1024
        ),
        name="halo",
    )(positions, masses, counts)


def density_kernel(
    cells, roll_ref, data_ref, out_ref,
    rel_ref, source_ref, move_ref, total_ref, place_ref, own_ref, target_ref, front_ref, back_ref, acc_ref, list_ref, list_sm, list_sem, *sums_refs,
):
    f32, i32 = jnp.float32, jnp.int32
    tiles = data_ref.shape[3] // cells
    slots = tiles * LANES
    wide = 4 * tiles
    list_tiles = list_ref.shape[0] - 1
    limits = tuple(min(wide, wide // 2 + more) for more in (-1, 0, 1))
    half_groups = GROUPS // 2
    half = 0.5

    masks = {}
    for sy in (-1, 0, 1):
        for sz in (-1, 0, 1):
            relation = 3 * (sy + 1) + sz + 1
            plane = sz + 1 if data_ref.shape[1] > 2 else 1 - abs(sz)
            parts = []
            for k in range(4):
                value = jnp.concatenate(
                    [data_ref[sy + 1, plane, k, pl.ds(t, cells, stride=tiles), :] for t in range(tiles)], axis=1
                )
                if sy != 0:
                    value = pltpu.roll(value, roll_ref[(sy + 1) // 2], 0)
                parts.append(value)
            y, x, z, mass = parts
            keep = mass > 0.0
            if sy == -1:
                keep = keep & (y >= half)
            elif sy == 1:
                keep = keep & (y <= half)
            if sz == -1:
                keep = keep & (z >= half)
            elif sz == 1:
                keep = keep & (z <= half)
            masks[sy, sz] = keep
            rel_ref[relation, 0] = 4.0 * (y + (sy - half))
            rel_ref[relation, 1] = 4.0 * (x - half)
            rel_ref[relation, 2] = 4.0 * (z + (sz - half))
            rel_ref[relation, 3] = mass
            if sy == 0 and sz == 0:
                own_y, own_x, own_z, own_valid = y, x, z, keep

    octants = []
    for ry, rz in RODS:
        inside = own_valid & ((own_y >= half) if ry else (own_y < half))
        inside = inside & ((own_z >= half) if rz else (own_z < half))
        octants.append(inside & (own_x < half))
        octants.append(inside & (own_x >= half))

    relations = [(sy, sz) for sy in (-1, 0, 1) for sz in (-1, 0, 1)]
    stacked = jnp.concatenate(
        [jnp.where(masks[r], 1.0, 0.0) for r in relations] + [jnp.where(m, 1.0, 0.0) for m in octants], axis=0
    ).astype(jnp.bfloat16)
    row = lax.broadcasted_iota(i32, (slots, slots + LANES), 0)
    col = lax.broadcasted_iota(i32, (slots, slots + LANES), 1)
    triangle = jnp.where((row <= col) | (col >= slots), 1.0, 0.0).astype(jnp.bfloat16)
    ranks = jnp.dot(stacked, triangle, preferred_element_type=f32).astype(i32)

    first = len(relations) * cells
    n_oct = len(octants) * cells
    cell_row = lax.broadcasted_iota(i32, (cells, LANES), 0)
    rods, words, ranking = [], [], []
    for r, (ry, rz) in enumerate(RODS):
        segments = [(0, 0), (2 * ry - 1, 0), (0, 2 * rz - 1), (2 * ry - 1, 2 * rz - 1)]
        starts, start = [], jnp.zeros((cells, LANES), i32)
        for sy, sz in segments:
            at = (3 * (sy + 1) + sz + 1) * cells
            starts.append(start)
            start = start + ranks[at:at + cells, slots:]
        rods.append((segments, starts, start))
        for side in range(2):
            turn = cells - 1 if side else 1
            other = pltpu.roll(cell_row, turn, 0)
            most = jnp.maximum(start, pltpu.roll(start, turn, 0))
            word = (r * cells + cell_row) + ((r * cells + other) << 7) + (cell_row << 14)
            words.append(word + (side << 19) + jnp.where(most > limits[-1] * LANES, 1 << 20, 0))
            ranking.append(sum(jnp.where(most > limit * LANES, n_oct, 0) for limit in limits[:-1]))
    word = jnp.concatenate(words, axis=0).astype(f32)

    totals = ranks[first:, slots:]
    groups = ((totals + (SUB - 1)) >> 3).astype(f32)
    oct_row = lax.broadcasted_iota(i32, (n_oct, LANES), 0)
    oct_lane = lax.broadcasted_iota(i32, (n_oct, LANES), 1)
    light = jnp.concatenate(ranking, axis=0)
    order = (light + oct_row).astype(f32)
    order_lane = jnp.sum(jnp.where(oct_row == oct_lane, order, 0.0), axis=0, keepdims=True)
    lower = jnp.where(order_lane < order, 1.0, 0.0).astype(jnp.bfloat16)
    base = jnp.dot(lower, groups.astype(jnp.bfloat16), preferred_element_type=f32)
    end = base + groups
    place = jnp.full((cells, slots), -1, i32)
    for o, inside in enumerate(octants):
        begin = base[o * cells:(o + 1) * cells].astype(i32)
        begin = jnp.concatenate([begin] * tiles, axis=1)
        rank = ranks[first + o * cells:first + (o + 1) * cells, :slots]
        place = jnp.where(inside, SUB * begin + rank - 1, place)
    for j in range(list_tiles):
        at = (oct_lane + (j * LANES - GROUPS)).astype(f32)
        held = jnp.sum(jnp.where((base <= at) & (at < end), word, 0.0), axis=0, keepdims=True)
        list_ref[j:j + 1, :] = held.astype(i32)
    counted = jnp.zeros((1, LANES), f32)
    for k in range(len(limits)):
        reached = jnp.sum(jnp.where(light <= k * n_oct, groups, 0.0), axis=0, keepdims=True)
        counted = jnp.where(oct_lane[:1] == k, reached, counted)
    list_ref[list_tiles:list_tiles + 1, :] = counted.astype(i32)

    for t in range(tiles):
        lanes = slice(t * LANES, (t + 1) * LANES)
        place_ref[t] = place[:, lanes]
        for f in range(3):
            own_ref[f * tiles + t] = rel_ref[4, f, :, lanes]
    copies = [
        pltpu.make_async_copy(list_ref.at[j], list_sm.at[pl.ds(j * LANES, LANES)], list_sem.at[j])
        for j in range(list_tiles + 1)
    ]
    lane = lax.broadcasted_iota(i32, (cells, LANES), 1)
    for r, (segments, starts, total) in enumerate(rods):
        held = slice(r * cells, (r + 1) * cells)
        total_ref[held] = total
        for k, (sy, sz) in enumerate(segments):
            at = (3 * (sy + 1) + sz + 1) * cells
            for t in range(tiles):
                lanes = slice(t * LANES, (t + 1) * LANES)
                word = lane << 10
                if k > 0:
                    shift = (k * slots + t * LANES + 1) + lane - starts[k] - ranks[at:at + cells, lanes]
                    word = word + jnp.where(masks[sy, sz][:, lanes], shift, 0)
                move_ref[k * tiles + t, held] = word
    for copy in copies:
        copy.start()

    lane8 = lax.broadcasted_iota(i32, (SUB, LANES), 1)
    blocks = len(RODS) * cells // SUB

    def ranked(words):
        step = 1
        while step < LANES:
            inner = lane8 < LANES - step
            turned = [pltpu.roll(w, LANES - step, 1) for w in words] + [jnp.zeros_like(lane8)]
            coming = [jnp.where(inner, turned[j], turned[j + 1]) for j in range(len(words))]
            words = [
                jnp.where((c & step) != 0, c, jnp.where((w & step) != 0, 0, w)) for c, w in zip(coming, words)
            ]
            step *= 2
        return words

    def settle(block):
        rod = block // (cells // SUB)
        top = pl.multiple_of((block - rod * (cells // SUB)) * SUB, SUB)
        held = pl.ds(pl.multiple_of(block * SUB, SUB), SUB)
        ry, rz = 2 * (rod >> 1), 2 * (rod & 1)
        segments = [4, 3 * ry + 1, 3 + rz, 3 * ry + rz]
        words = [move_ref[j, held] for j in range(wide)]
        words = words[:tiles - 1] + ranked(words[tiles - 1:])
        origin = [w >> 10 for w in words]
        raw = [
            [
                rel_ref[segments[j // tiles], f, pl.ds(top, SUB), (j % tiles) * LANES:(j % tiles + 1) * LANES]
                for j in range(wide)
            ]
            for f in range(4)
        ]
        data = [[] for _ in range(4)]
        for j in range(wide):
            for f in range(4):
                here = raw[f][j]
                if j >= tiles:
                    here = jnp.take_along_axis(here, origin[j], axis=1, mode="promise_in_bounds")
                if tiles - 1 <= j < wide - 1:
                    after = jnp.take_along_axis(raw[f][j + 1], origin[j], axis=1, mode="promise_in_bounds")
                    here = jnp.where(origin[j] >= lane8, here, after)
                data[f].append(here)
        step = LANES
        while step < wide * LANES:
            q = step // LANES
            coming = [(w & step) != 0 for w in words[q:]]
            leaving = [(w & step) != 0 for w in words]
            kept = [jnp.where(leaving[j], 0, words[j]) for j in range(wide)]
            words = [jnp.where(coming[j], words[j + q], kept[j]) for j in range(wide - q)] + kept[wide - q:]
            data = [[jnp.where(coming[j], a[j + q], a[j]) for j in range(wide - q)] + a[wide - q:] for a in data]
            step *= 2
        total = total_ref[held]
        for j in range(wide):
            for f in range(3):
                source_ref[f * wide + j, held] = data[f][j]
            source_ref[3 * wide + j, held] = jnp.where(lane8 + j * LANES < total, data[3][j], 0.0)

    together = next(n for n in (4, 2, 1) if blocks % n == 0)

    def settle_some(step, carry):
        for k in range(together):
            settle(step * together + k)
        return carry

    lax.fori_loop(0, blocks // together, settle_some, 0)
    for copy in copies:
        copy.wait()

    sub_row = lax.broadcasted_iota(i32, (SUB, LANES), 0)

    def entries(body):
        return [list_sm[(body + 1) * GROUPS + k] for k in range(GROUPS)]

    def chosen(word, g):
        cell = (word >> 14) & 31
        rows = sub_row + g * SUB
        return cell, [place_ref[t, pl.ds(cell, SUB, stride=0)] == rows for t in range(tiles)]

    def gathered(word, g):
        cell, mask = chosen(word, g)
        for f in range(3):
            value = sum(
                jnp.where(mask[t], own_ref[f * tiles + t, pl.ds(cell, SUB, stride=0)], 0.0) for t in range(tiles)
            )
            yield f, jnp.broadcast_to(jnp.sum(value, axis=1, keepdims=True), (SUB, LANES))

    def gather(body, first, words, held):
        for k, word in enumerate(words):
            for f, value in gathered(word, body * GROUPS + first + k):
                held[3 * k + f] = value

    def scatter(body):
        for k, word in enumerate(entries(body)):
            cell, mask = chosen(word, body * GROUPS + k)
            total = jnp.sum(acc_ref[k], axis=1, keepdims=True)
            for t in range(tiles):
                at = cell * tiles + t
                held = sums_refs[k % len(sums_refs)]
                held[at] = held[at] + jnp.where(mask[t], total, 0.0)

    def part(line, at, ty, tx, tz, acc):
        y, x, z, mass = (source_ref[f * wide + at, pl.ds(line, SUB, stride=0)] for f in range(4))
        dy, dx, dz = y - ty, x - tx, z - tz
        squared = dy * dy + dx * dx + dz * dz
        q = pl.reciprocal(lax.rsqrt(squared))
        outer = jnp.maximum(2.0 - q, 0.0)
        value = jnp.minimum(4.0 - 3.0 * (squared * outer), outer * outer * outer)
        return acc + mass * value

    def compute(targets, k, word, begin, finish, acc):
        line, other = word & 127, (word >> 7) & 127
        offset = jnp.where((word & (1 << 19)) != 0, -4.0, 4.0)
        ty, tx, tz = targets
        moved = tx + offset
        for at in range(begin, finish):
            acc = part(line, at, ty, tx, tz, acc)
            acc = part(other, at, ty, moved, tz, acc)
        acc_ref[k] = acc

    for held in sums_refs:
        held[...] = jnp.zeros(held.shape, f32)
    acc_ref[...] = jnp.zeros(acc_ref.shape, f32)
    reached = [list_sm[list_tiles * LANES + k] for k in range(len(limits))]
    bodies = (reached[-1] + (GROUPS - 1)) // GROUPS
    bounds = [0] + [n // GROUPS for n in reached[:-1]] + [bodies]
    gather(0, 0, entries(0)[:half_groups], front_ref)

    def body_step(limit, body, carry):
        words = entries(body)
        scatter(body - 1)
        gather(body, half_groups, words[half_groups:], back_ref)
        zero = jnp.zeros((SUB, LANES), f32)
        for k, word in enumerate(words[:half_groups]):
            compute([front_ref[3 * k + f] for f in range(3)], k, word, 0, limit, zero)
        if limit == limits[-1]:
            target_ref[:3 * half_groups] = front_ref[...]
            target_ref[3 * half_groups:] = back_ref[...]
        gather(body + 1, 0, entries(body + 1)[:half_groups], front_ref)
        for k, word in enumerate(words[half_groups:]):
            compute([back_ref[3 * k + f] for f in range(3)], half_groups + k, word, 0, limit, zero)
        if limit != limits[-1]:
            return carry
        flags = words[0]
        for word in words[1:]:
            flags = flags | word

        @pl.when((flags & (1 << 20)) != 0)
        def _():
            def far_step(k, carry):
                word = list_sm[(body + 1) * GROUPS + k]

                @pl.when((word & (1 << 20)) != 0)
                def _():
                    compute([target_ref[3 * k + f] for f in range(3)], k, word, limit, wide, acc_ref[k])

                return carry

            lax.fori_loop(0, GROUPS, far_step, 0)

        return carry

    for limit, begin, finish in zip(limits, bounds, bounds[1:]):
        lax.fori_loop(begin, finish, functools.partial(body_step, limit), 0)
    scatter(bodies - 1)
    for at in range(cells * tiles):
        out_ref[at:at + 1, :] = jnp.sum(sum(held[at] for held in sums_refs), axis=0, keepdims=True) * (16.0 / 3.141592653589793)


def shards(positions, masses, counts, shear_offset):
    cells_y, cells, cells_z, slots = masses.shape
    assert cells_y == 1 and cells_z == 1 and slots % LANES == 0
    tiles = slots // LANES
    rows = cells * tiles
    padded = halo(positions.reshape(3, rows, LANES), masses.reshape(rows, LANES), counts.reshape(cells))
    offset = shear_offset[0]
    shear_index = lax.axis_index("shear")
    cycle = lax.axis_size("shear")
    low = jnp.where(shear_index == 0, offset, 0) % cells
    high = jnp.where(shear_index == cycle - 1, -offset, 0) % cells
    rolls = jnp.stack([low, high]).astype(jnp.int32)

    octants = 2 * len(RODS)
    most_groups = cells * (slots // SUB + octants - 1)
    list_tiles = -(-(most_groups + 3 * GROUPS) // LANES)
    wide = 4 * slots
    smem = pl.BlockSpec(memory_space=pltpu.SMEM)
    vmem = pl.BlockSpec(memory_space=pltpu.VMEM)
    density = pl.pallas_call(
        functools.partial(density_kernel, cells),
        out_shape=jax.ShapeDtypeStruct((rows, LANES), jnp.float32),
        in_specs=[smem, vmem],
        out_specs=vmem,
        scratch_shapes=[
            pltpu.VMEM((9, 4, cells, slots), jnp.float32),
            pltpu.VMEM((4 * wide // LANES, len(RODS) * cells, LANES), jnp.float32),
            pltpu.VMEM((wide // LANES, len(RODS) * cells, LANES), jnp.int32),
            pltpu.VMEM((len(RODS) * cells, LANES), jnp.int32),
            pltpu.VMEM((tiles, cells, LANES), jnp.int32),
            pltpu.VMEM((3 * tiles, cells, LANES), jnp.float32),
            pltpu.VMEM((3 * GROUPS, SUB, LANES), jnp.float32),
            pltpu.VMEM((3 * GROUPS // 2, SUB, LANES), jnp.float32),
            pltpu.VMEM((3 * GROUPS // 2, SUB, LANES), jnp.float32),
            pltpu.VMEM((GROUPS, SUB, LANES), jnp.float32),
            pltpu.VMEM((list_tiles + 1, LANES), jnp.int32),
            pltpu.SMEM(((list_tiles + 1) * LANES,), jnp.int32),
            pltpu.SemaphoreType.DMA((list_tiles + 1,)),
        ] + 4 * [pltpu.VMEM((rows, SUB, LANES), jnp.float32)],
        compiler_params=pltpu.CompilerParams(vmem_limit_bytes=12 * 1024 * 1024),
        name="density",
    )(rolls, padded)
    return density.reshape(masses.shape)


def solution(mesh):
    in_specs = (
        P(None, "shear", None, "cross", None),
        P("shear", None, "cross", None),
        P("shear", None, "cross"),
        P(),
    )
    out_specs = P("shear", None, "cross", None)
    return jax.shard_map(shards, mesh=mesh, in_specs=in_specs, out_specs=out_specs, check_vma=False)
```

```python
import functools
import jax
import jax.numpy as jnp
from jax import lax
from jax.experimental import pallas as pl
from jax.experimental.pallas import tpu as pltpu
from jax.sharding import PartitionSpec as P

LANES = 128
SUB = 8
GROUPS = 8
RODS = ((0, 0), (0, 1), (1, 0), (1, 1))


def halo_kernel(
    pos_ref, mass_ref, counts_ref, out_ref, held_ref, counts_sm, send_sems, recv_sems, local_sems,
):
    shear, cross = lax.axis_index("shear"), lax.axis_index("cross")
    rows, planes = lax.axis_size("shear"), lax.axis_size("cross")
    mesh_ids = pl.DeviceIdType.MESH
    sides = (0, 2) if planes > 2 else (0,)
    along_y = [(lax.rem(shear + rows - step, rows), cross) for step in (-1, 1)]
    along_z = [(shear, lax.rem(cross + planes - step, planes)) for step in (-1, 1)][:len(sides)]
    barrier = pltpu.get_barrier_semaphore()
    for device in along_y + along_z:
        pl.semaphore_signal(barrier, inc=1, device_id=device, device_id_type=mesh_ids)
    own = out_ref.at[1, 1]
    loads = [
        pltpu.make_async_copy(counts_ref, counts_sm, local_sems.at[0]),
        pltpu.make_async_copy(mass_ref, held_ref, local_sems.at[1]),
        pltpu.make_async_copy(pos_ref, own.at[pl.ds(0, 3)], local_sems.at[2]),
    ]
    for copy in loads:
        copy.start()
    for copy in loads[:2]:
        copy.wait()
    lines, cells = held_ref.shape[0], counts_sm.shape[0]
    tiles = lines // cells
    line = lax.broadcasted_iota(jnp.int32, (lines, LANES), 0)
    slot = lax.broadcasted_iota(jnp.int32, (lines, LANES), 1) + LANES * lax.rem(line, tiles)
    limit = jnp.zeros((lines, LANES), jnp.int32)
    for cell in range(cells):
        inside = (line >= cell * tiles) & (line < (cell + 1) * tiles)
        limit = jnp.where(inside, counts_sm[cell], limit)
    own[3] = jnp.where(slot < limit, held_ref[...], 0.0)
    loads[2].wait()
    pl.semaphore_wait(barrier, len(along_y) + len(along_z))

    def sent(source, y, z, device):
        at = 3 * y + z
        copy = pltpu.make_async_remote_copy(
            src_ref=source,
            dst_ref=out_ref.at[y, z],
            send_sem=send_sems.at[at],
            recv_sem=recv_sems.at[at],
            device_id=device,
            device_id_type=mesh_ids,
        )
        copy.start()
        return copy

    rows_sent = [sent(own, y, 1, along_y[k]) for k, y in enumerate((0, 2))]
    planes_sent = [sent(own, 1, z, along_z[k]) for k, z in enumerate(sides)]
    for k, y in ((1, 2), (0, 0)):
        rows_sent[k].wait_recv()
        for j, z in enumerate(sides):
            planes_sent.append(sent(out_ref.at[y, 1], y, z, along_z[j]))
    for copy in rows_sent:
        copy.wait_send()
    for copy in planes_sent:
        copy.wait()


def halo(positions, masses, counts):
    lines = masses.shape[0]
    depth = 3 if lax.axis_size("cross") > 2 else 2
    return pl.pallas_call(
        halo_kernel,
        out_shape=jax.ShapeDtypeStruct((3, depth, 4, lines, LANES), masses.dtype),
        in_specs=[pl.BlockSpec(memory_space=pl.ANY)] * 3,
        out_specs=pl.BlockSpec(memory_space=pltpu.VMEM),
        scratch_shapes=[
            pltpu.VMEM((lines, LANES), jnp.float32),
            pltpu.SMEM(counts.shape, jnp.int32),
            pltpu.SemaphoreType.DMA((9,)),
            pltpu.SemaphoreType.DMA((9,)),
            pltpu.SemaphoreType.DMA((3,)),
        ],
        compiler_params=pltpu.CompilerParams(
            collective_id=0, has_side_effects=True, vmem_limit_bytes=4 * 1024 * 1024
        ),
        name="halo",
    )(positions, masses, counts)


def density_kernel(
    cells, roll_ref, data_ref, out_ref,
    rel_ref, source_ref, move_ref, total_ref, place_ref, own_ref, target_ref, front_ref, back_ref, acc_ref, list_ref, list_sm, list_sem, *sums_refs,
):
    f32, i32 = jnp.float32, jnp.int32
    tiles = data_ref.shape[3] // cells
    slots = tiles * LANES
    wide = 4 * tiles
    list_tiles = list_ref.shape[0] - 1
    limits = tuple(min(wide, wide // 2 + more) for more in (-1, 0, 1))
    half_groups = GROUPS // 2
    half = 0.5

    masks = {}
    for sy in (-1, 0, 1):
        for sz in (-1, 0, 1):
            relation = 3 * (sy + 1) + sz + 1
            plane = sz + 1 if data_ref.shape[1] > 2 else 1 - abs(sz)
            parts = []
            for k in range(4):
                value = jnp.concatenate(
                    [data_ref[sy + 1, plane, k, pl.ds(t, cells, stride=tiles), :] for t in range(tiles)], axis=1
                )
                if sy != 0:
                    value = pltpu.roll(value, roll_ref[(sy + 1) // 2], 0)
                parts.append(value)
            y, x, z, mass = parts
            keep = mass > 0.0
            if sy == -1:
                keep = keep & (y >= half)
            elif sy == 1:
                keep = keep & (y <= half)
            if sz == -1:
                keep = keep & (z >= half)
            elif sz == 1:
                keep = keep & (z <= half)
            masks[sy, sz] = keep
            rel_ref[relation, 0] = 4.0 * (y + (sy - half))
            rel_ref[relation, 1] = 4.0 * (x - half)
            rel_ref[relation, 2] = 4.0 * (z + (sz - half))
            rel_ref[relation, 3] = mass
            if sy == 0 and sz == 0:
                own_y, own_x, own_z, own_valid = y, x, z, keep

    octants = []
    for ry, rz in RODS:
        inside = own_valid & ((own_y >= half) if ry else (own_y < half))
        inside = inside & ((own_z >= half) if rz else (own_z < half))
        octants.append(inside & (own_x < half))
        octants.append(inside & (own_x >= half))

    relations = [(sy, sz) for sy in (-1, 0, 1) for sz in (-1, 0, 1)]
    stacked = jnp.concatenate(
        [jnp.where(masks[r], 1.0, 0.0) for r in relations] + [jnp.where(m, 1.0, 0.0) for m in octants], axis=0
    ).astype(jnp.bfloat16)
    row = lax.broadcasted_iota(i32, (slots, slots + LANES), 0)
    col = lax.broadcasted_iota(i32, (slots, slots + LANES), 1)
    triangle = jnp.where((row <= col) | (col >= slots), 1.0, 0.0).astype(jnp.bfloat16)
    ranks = jnp.dot(stacked, triangle, preferred_element_type=f32).astype(i32)

    first = len(relations) * cells
    n_oct = len(octants) * cells
    cell_row = lax.broadcasted_iota(i32, (cells, LANES), 0)
    rods, words, ranking = [], [], []
    for r, (ry, rz) in enumerate(RODS):
        segments = [(0, 0), (2 * ry - 1, 0), (0, 2 * rz - 1), (2 * ry - 1, 2 * rz - 1)]
        starts, start = [], jnp.zeros((cells, LANES), i32)
        for sy, sz in segments:
            at = (3 * (sy + 1) + sz + 1) * cells
            starts.append(start)
            start = start + ranks[at:at + cells, slots:]
        rods.append((segments, starts, start))
        for side in range(2):
            turn = cells - 1 if side else 1
            other = pltpu.roll(cell_row, turn, 0)
            most = jnp.maximum(start, pltpu.roll(start, turn, 0))
            word = (r * cells + cell_row) + ((r * cells + other) << 7) + (cell_row << 14)
            words.append(word + (side << 19) + jnp.where(most > limits[-1] * LANES, 1 << 20, 0))
            ranking.append(sum(jnp.where(most > limit * LANES, n_oct, 0) for limit in limits[:-1]))
    word = jnp.concatenate(words, axis=0).astype(f32)

    totals = ranks[first:, slots:]
    groups = ((totals + (SUB - 1)) >> 3).astype(f32)
    oct_row = lax.broadcasted_iota(i32, (n_oct, LANES), 0)
    oct_lane = lax.broadcasted_iota(i32, (n_oct, LANES), 1)
    light = jnp.concatenate(ranking, axis=0)
    order = (light + oct_row).astype(f32)
    order_lane = jnp.sum(jnp.where(oct_row == oct_lane, order, 0.0), axis=0, keepdims=True)
    lower = jnp.where(order_lane < order, 1.0, 0.0).astype(jnp.bfloat16)
    base = jnp.dot(lower, groups.astype(jnp.bfloat16), preferred_element_type=f32)
    end = base + groups
    place = jnp.full((cells, slots), -1, i32)
    for o, inside in enumerate(octants):
        begin = base[o * cells:(o + 1) * cells].astype(i32)
        begin = jnp.concatenate([begin] * tiles, axis=1)
        rank = ranks[first + o * cells:first + (o + 1) * cells, :slots]
        place = jnp.where(inside, SUB * begin + rank - 1, place)
    for j in range(list_tiles):
        at = (oct_lane + (j * LANES - GROUPS)).astype(f32)
        held = jnp.sum(jnp.where((base <= at) & (at < end), word, 0.0), axis=0, keepdims=True)
        list_ref[j:j + 1, :] = held.astype(i32)
    counted = jnp.zeros((1, LANES), f32)
    for k in range(len(limits)):
        reached = jnp.sum(jnp.where(light <= k * n_oct, groups, 0.0), axis=0, keepdims=True)
        counted = jnp.where(oct_lane[:1] == k, reached, counted)
    list_ref[list_tiles:list_tiles + 1, :] = counted.astype(i32)

    for t in range(tiles):
        lanes = slice(t * LANES, (t + 1) * LANES)
        place_ref[t] = place[:, lanes]
        for f in range(3):
            own_ref[f * tiles + t] = rel_ref[4, f, :, lanes]
    copies = [
        pltpu.make_async_copy(list_ref.at[j], list_sm.at[pl.ds(j * LANES, LANES)], list_sem.at[j])
        for j in range(list_tiles + 1)
    ]
    lane = lax.broadcasted_iota(i32, (cells, LANES), 1)
    for r, (segments, starts, total) in enumerate(rods):
        held = slice(r * cells, (r + 1) * cells)
        total_ref[held] = total
        for k, (sy, sz) in enumerate(segments):
            at = (3 * (sy + 1) + sz + 1) * cells
            for t in range(tiles):
                lanes = slice(t * LANES, (t + 1) * LANES)
                word = lane << 10
                if k > 0:
                    shift = (k * slots + t * LANES + 1) + lane - starts[k] - ranks[at:at + cells, lanes]
                    word = word + jnp.where(masks[sy, sz][:, lanes], shift, 0)
                move_ref[k * tiles + t, held] = word
    for copy in copies:
        copy.start()

    lane8 = lax.broadcasted_iota(i32, (SUB, LANES), 1)
    blocks = len(RODS) * cells // SUB

    def ranked(words):
        step = 1
        while step < LANES:
            inner = lane8 < LANES - step
            turned = [pltpu.roll(w, LANES - step, 1) for w in words] + [jnp.zeros_like(lane8)]
            coming = [jnp.where(inner, turned[j], turned[j + 1]) for j in range(len(words))]
            words = [
                jnp.where((c & step) != 0, c, jnp.where((w & step) != 0, 0, w)) for c, w in zip(coming, words)
            ]
            step *= 2
        return words

    def settle(block):
        rod = block // (cells // SUB)
        top = pl.multiple_of((block - rod * (cells // SUB)) * SUB, SUB)
        held = pl.ds(pl.multiple_of(block * SUB, SUB), SUB)
        ry, rz = 2 * (rod >> 1), 2 * (rod & 1)
        segments = [4, 3 * ry + 1, 3 + rz, 3 * ry + rz]
        words = [move_ref[j, held] for j in range(wide)]
        words = words[:tiles - 1] + ranked(words[tiles - 1:])
        origin = [w >> 10 for w in words]
        raw = [
            [
                rel_ref[segments[j // tiles], f, pl.ds(top, SUB), (j % tiles) * LANES:(j % tiles + 1) * LANES]
                for j in range(wide)
            ]
            for f in range(4)
        ]
        data = [[] for _ in range(4)]
        for j in range(wide):
            for f in range(4):
                here = raw[f][j]
                if j >= tiles:
                    here = jnp.take_along_axis(here, origin[j], axis=1, mode="promise_in_bounds")
                if tiles - 1 <= j < wide - 1:
                    after = jnp.take_along_axis(raw[f][j + 1], origin[j], axis=1, mode="promise_in_bounds")
                    here = jnp.where(origin[j] >= lane8, here, after)
                data[f].append(here)
        step = LANES
        while step < wide * LANES:
            q = step // LANES
            coming = [(w & step) != 0 for w in words[q:]]
            leaving = [(w & step) != 0 for w in words]
            kept = [jnp.where(leaving[j], 0, words[j]) for j in range(wide)]
            words = [jnp.where(coming[j], words[j + q], kept[j]) for j in range(wide - q)] + kept[wide - q:]
            data = [[jnp.where(coming[j], a[j + q], a[j]) for j in range(wide - q)] + a[wide - q:] for a in data]
            step *= 2
        total = total_ref[held]
        for j in range(wide):
            for f in range(3):
                source_ref[f * wide + j, held] = data[f][j]
            source_ref[3 * wide + j, held] = jnp.where(lane8 + j * LANES < total, data[3][j], 0.0)

    together = next(n for n in (4, 2, 1) if blocks % n == 0)

    def settle_some(step, carry):
        for k in range(together):
            settle(step * together + k)
        return carry

    lax.fori_loop(0, blocks // together, settle_some, 0)
    for copy in copies:
        copy.wait()

    sub_row = lax.broadcasted_iota(i32, (SUB, LANES), 0)

    def entries(body):
        return [list_sm[(body + 1) * GROUPS + k] for k in range(GROUPS)]

    def chosen(word, g):
        cell = (word >> 14) & 31
        rows = sub_row + g * SUB
        return cell, [place_ref[t, pl.ds(cell, SUB, stride=0)] == rows for t in range(tiles)]

    def gathered(word, g):
        cell, mask = chosen(word, g)
        for f in range(3):
            value = sum(
                jnp.where(mask[t], own_ref[f * tiles + t, pl.ds(cell, SUB, stride=0)], 0.0) for t in range(tiles)
            )
            yield f, jnp.broadcast_to(jnp.sum(value, axis=1, keepdims=True), (SUB, LANES))

    def gather(body, first, words, held):
        for k, word in enumerate(words):
            for f, value in gathered(word, body * GROUPS + first + k):
                held[3 * k + f] = value

    def scatter(body):
        for k, word in enumerate(entries(body)):
            cell, mask = chosen(word, body * GROUPS + k)
            total = jnp.sum(acc_ref[k], axis=1, keepdims=True)
            for t in range(tiles):
                at = cell * tiles + t
                held = sums_refs[k % len(sums_refs)]
                held[at] = held[at] + jnp.where(mask[t], total, 0.0)

    def part(line, at, ty, tx, tz, acc):
        y, x, z, mass = (source_ref[f * wide + at, pl.ds(line, SUB, stride=0)] for f in range(4))
        dy, dx, dz = y - ty, x - tx, z - tz
        squared = dy * dy + dx * dx + dz * dz
        q = pl.reciprocal(lax.rsqrt(squared))
        outer = jnp.maximum(2.0 - q, 0.0)
        value = jnp.minimum(4.0 - 3.0 * (squared * outer), outer * outer * outer)
        return acc + mass * value

    def compute(targets, k, word, begin, finish, acc):
        line, other = word & 127, (word >> 7) & 127
        offset = jnp.where((word & (1 << 19)) != 0, -4.0, 4.0)
        ty, tx, tz = targets
        moved = tx + offset
        for at in range(begin, finish):
            acc = part(line, at, ty, tx, tz, acc)
            acc = part(other, at, ty, moved, tz, acc)
        acc_ref[k] = acc

    for held in sums_refs:
        held[...] = jnp.zeros(held.shape, f32)
    acc_ref[...] = jnp.zeros(acc_ref.shape, f32)
    reached = [list_sm[list_tiles * LANES + k] for k in range(len(limits))]
    bodies = (reached[-1] + (GROUPS - 1)) // GROUPS
    bounds = [0] + [n // GROUPS for n in reached[:-1]] + [bodies]
    gather(0, 0, entries(0)[:half_groups], front_ref)

    def body_step(limit, body, carry):
        words = entries(body)
        scatter(body - 1)
        gather(body, half_groups, words[half_groups:], back_ref)
        zero = jnp.zeros((SUB, LANES), f32)
        for k, word in enumerate(words[:half_groups]):
            compute([front_ref[3 * k + f] for f in range(3)], k, word, 0, limit, zero)
        if limit == limits[-1]:
            target_ref[:3 * half_groups] = front_ref[...]
            target_ref[3 * half_groups:] = back_ref[...]
        gather(body + 1, 0, entries(body + 1)[:half_groups], front_ref)
        for k, word in enumerate(words[half_groups:]):
            compute([back_ref[3 * k + f] for f in range(3)], half_groups + k, word, 0, limit, zero)
        if limit != limits[-1]:
            return carry
        flags = words[0]
        for word in words[1:]:
            flags = flags | word

        @pl.when((flags & (1 << 20)) != 0)
        def _():
            def far_step(k, carry):
                word = list_sm[(body + 1) * GROUPS + k]

                @pl.when((word & (1 << 20)) != 0)
                def _():
                    compute([target_ref[3 * k + f] for f in range(3)], k, word, limit, wide, acc_ref[k])

                return carry

            lax.fori_loop(0, GROUPS, far_step, 0)

        return carry

    for limit, begin, finish in zip(limits, bounds, bounds[1:]):
        lax.fori_loop(begin, finish, functools.partial(body_step, limit), 0)
    scatter(bodies - 1)
    for at in range(cells * tiles):
        out_ref[at:at + 1, :] = jnp.sum(sum(held[at] for held in sums_refs), axis=0, keepdims=True) * (16.0 / 3.141592653589793)


def shards(positions, masses, counts, shear_offset):
    cells_y, cells, cells_z, slots = masses.shape
    assert cells_y == 1 and cells_z == 1 and slots % LANES == 0
    tiles = slots // LANES
    rows = cells * tiles
    padded = halo(positions.reshape(3, rows, LANES), masses.reshape(rows, LANES), counts.reshape(cells))
    offset = shear_offset[0]
    shear_index = lax.axis_index("shear")
    cycle = lax.axis_size("shear")
    low = jnp.where(shear_index == 0, offset, 0) % cells
    high = jnp.where(shear_index == cycle - 1, -offset, 0) % cells
    rolls = jnp.stack([low, high]).astype(jnp.int32)

    octants = 2 * len(RODS)
    most_groups = cells * (slots // SUB + octants - 1)
    list_tiles = -(-(most_groups + 3 * GROUPS) // LANES)
    wide = 4 * slots
    smem = pl.BlockSpec(memory_space=pltpu.SMEM)
    vmem = pl.BlockSpec(memory_space=pltpu.VMEM)
    density = pl.pallas_call(
        functools.partial(density_kernel, cells),
        out_shape=jax.ShapeDtypeStruct((rows, LANES), jnp.float32),
        in_specs=[smem, vmem],
        out_specs=vmem,
        scratch_shapes=[
            pltpu.VMEM((9, 4, cells, slots), jnp.float32),
            pltpu.VMEM((4 * wide // LANES, len(RODS) * cells, LANES), jnp.float32),
            pltpu.VMEM((wide // LANES, len(RODS) * cells, LANES), jnp.int32),
            pltpu.VMEM((len(RODS) * cells, LANES), jnp.int32),
            pltpu.VMEM((tiles, cells, LANES), jnp.int32),
            pltpu.VMEM((3 * tiles, cells, LANES), jnp.float32),
            pltpu.VMEM((3 * GROUPS, SUB, LANES), jnp.float32),
            pltpu.VMEM((3 * GROUPS // 2, SUB, LANES), jnp.float32),
            pltpu.VMEM((3 * GROUPS // 2, SUB, LANES), jnp.float32),
            pltpu.VMEM((GROUPS, SUB, LANES), jnp.float32),
            pltpu.VMEM((list_tiles + 1, LANES), jnp.int32),
            pltpu.SMEM(((list_tiles + 1) * LANES,), jnp.int32),
            pltpu.SemaphoreType.DMA((list_tiles + 1,)),
        ] + 2 * [pltpu.VMEM((rows, SUB, LANES), jnp.float32)],
        compiler_params=pltpu.CompilerParams(vmem_limit_bytes=12 * 1024 * 1024),
        name="density",
    )(rolls, padded)
    return density.reshape(masses.shape)


def solution(mesh):
    in_specs = (
        P(None, "shear", None, "cross", None),
        P("shear", None, "cross", None),
        P("shear", None, "cross"),
        P(),
    )
    out_specs = P("shear", None, "cross", None)
    return jax.shard_map(shards, mesh=mesh, in_specs=in_specs, out_specs=out_specs, check_vma=False)
```
